64 devices in a mesh: rep: 4 (over x, y), pool: 16 (over z, core).
Axes of the slice: x: 2, y: 2, z: 8, core: 2. Of those that a mesh axis runs over, the one named last changes fastest.
The devices are a block of a 4x4x8 slice.
Arguments:
- kv_pool: bfloat16 [2, 4096, 2, 16, 36, 64], P(None, ('rep', 'pool')), parts along dimension 1
- page_idx: int32 [16, 64, 4], P(None, ('rep', 'pool')), parts along dimension 1
- tok_hidden: bfloat16 [64, 64, 2304], P(('rep', 'pool')), parts along dimension 0
- attn_norm: bfloat16 [2, 2304], replicated
- w_query: bfloat16 [2, 2304, 2304], replicated
- w_key: bfloat16 [2, 2304, 2304], replicated
- w_value: bfloat16 [2, 2304, 2304], replicated
- w_out: bfloat16 [2, 2304, 2304], replicated
- mlp_norm: bfloat16 [2, 2304], replicated
- w_gate: bfloat16 [2, 2304, 5760], replicated
- w_up: bfloat16 [2, 2304, 5760], replicated
- w_down: bfloat16 [2, 5760, 2304], replicated
Outputs:
- output: bfloat16 [64, 64, 2304], P(('rep', 'pool')), parts along dimension 0
There are 4 independent parts. The reference program is written for one: setup_inputs(seed, part) draws one part's arguments, and reference() takes and returns one part's arrays. A program takes and returns all parts, laid end to end along the dimension named above; an argument that names none is the same for every part.
All inputs are finite; a program needn't handle non-finite values.
Results may differ from the reference program's by a relative error of at most 0.0166935.
Values are sent between devices in bfloat16 or wider.
A program may use at most 768 MiB of HBM per device.

```python
import math
import jax
import jax.numpy as jnp
from jax import lax

GROUP = 16
LAYERS = 2
TOKENS = 64
PAGE_LEN = 16
SLOTS = 4
POOL_PAGES = 64
HIDDEN = 2304
NUM_HEADS = 36
HEAD_DIM = 64
FF_DIM = 5760
ROPE_BASE = 10000

PREFIX = GROUP * SLOTS * PAGE_LEN
ATTN_WIDTH = NUM_HEADS * HEAD_DIM


def setup_inputs(seed: int = 0, part: int = 0) -> dict:
    part_key = jax.random.fold_in(jax.random.key(seed), part)
    pool_key, idx_key, hid_key = jax.random.split(part_key, 3)
    weight_keys = jax.random.split(jax.random.key(seed + 1), 9)
    kv_pool = jax.random.normal(pool_key, (LAYERS, GROUP * POOL_PAGES, 2, PAGE_LEN, NUM_HEADS, HEAD_DIM), jnp.float32).astype(jnp.bfloat16)
    owner_keys = jax.random.split(idx_key, GROUP)
    page_perm = jax.vmap(lambda owner_key: jax.random.permutation(owner_key, POOL_PAGES))(owner_keys)
    chosen = page_perm[:, : GROUP * SLOTS].reshape(GROUP, GROUP, SLOTS)
    page_idx = jnp.transpose(chosen, (1, 0, 2)).astype(jnp.int32)
    tok_hidden = jax.random.normal(hid_key, (GROUP, TOKENS, HIDDEN), jnp.float32).astype(jnp.bfloat16)

    def make_weight(key, shape, fan_in, gain):
        return (jax.random.normal(key, shape, jnp.float32) * (gain / math.sqrt(fan_in))).astype(jnp.bfloat16)

    def make_gain(key):
        return (1.0 + 0.3 * jax.random.normal(key, (LAYERS, HIDDEN), jnp.float32)).astype(jnp.bfloat16)

    return {
        'kv_pool': kv_pool,
        'page_idx': page_idx,
        'tok_hidden': tok_hidden,
        'attn_norm': make_gain(weight_keys[0]),
        'w_query': make_weight(weight_keys[1], (LAYERS, HIDDEN, ATTN_WIDTH), HIDDEN, 2.5),
        'w_key': make_weight(weight_keys[2], (LAYERS, HIDDEN, ATTN_WIDTH), HIDDEN, 1.0),
        'w_value': make_weight(weight_keys[3], (LAYERS, HIDDEN, ATTN_WIDTH), HIDDEN, 1.0),
        'w_out': make_weight(weight_keys[4], (LAYERS, ATTN_WIDTH, HIDDEN), ATTN_WIDTH, 1.0),
        'mlp_norm': make_gain(weight_keys[5]),
        'w_gate': make_weight(weight_keys[6], (LAYERS, HIDDEN, FF_DIM), HIDDEN, 1.0),
        'w_up': make_weight(weight_keys[7], (LAYERS, HIDDEN, FF_DIM), HIDDEN, 1.0),
        'w_down': make_weight(weight_keys[8], (LAYERS, FF_DIM, HIDDEN), FF_DIM, 1.0),
    }


def rms_norm(vals, gain):
    vals_f = vals.astype(jnp.float32)
    inv_rms = lax.rsqrt(jnp.mean(vals_f * vals_f, axis=-1, keepdims=True) + 1e-6)
    return (vals_f * inv_rms * gain.astype(jnp.float32)).astype(jnp.bfloat16)


def rope_tables():
    positions = (PREFIX + jnp.arange(TOKENS)).astype(jnp.float32)
    exponent = jnp.arange(HEAD_DIM // 2).astype(jnp.float32) * (-2.0 / HEAD_DIM)
    inv_freq = jnp.power(float(ROPE_BASE), exponent)
    angles = positions[:, None] * inv_freq[None, :]
    return jnp.cos(angles)[:, None, :], jnp.sin(angles)[:, None, :]


def apply_rope(proj, cosine, sine):
    half = HEAD_DIM // 2
    first = proj[..., :half]
    second = proj[..., half:]
    return jnp.concatenate([first * cosine - second * sine, second * cosine + first * sine], axis=-1)


def reference(kv_pool, page_idx, tok_hidden, attn_norm, w_query, w_key, w_value, w_out, mlp_norm, w_gate, w_up, w_down):
    cosine, sine = rope_tables()
    owner_base = (jnp.arange(GROUP) * POOL_PAGES)[:, None]
    causal = jnp.arange(TOKENS)[None, :] <= jnp.arange(TOKENS)[:, None]
    visible = jnp.concatenate([jnp.full((TOKENS, PREFIX), True), causal], axis=1)
    scale = 1.0 / math.sqrt(HEAD_DIM)
    layer_stack = (kv_pool, attn_norm, w_query, w_key, w_value, w_out, mlp_norm, w_gate, w_up, w_down)
    head_shape = (TOKENS, NUM_HEADS, HEAD_DIM)

    def one_request(request_in):
        tok_rows, page_rows = request_in
        flat_pages = (page_rows + owner_base).reshape(GROUP * SLOTS)

        def layer_step(hidden, layer_in):
            layer_pool, gain_attn, q_weight, k_weight, v_weight, o_weight, gain_mlp, gate_weight, up_weight, down_weight = layer_in
            fetched = layer_pool[flat_pages]
            key_pre = fetched[:, 0].reshape(PREFIX, NUM_HEADS, HEAD_DIM)
            val_pre = fetched[:, 1].reshape(PREFIX, NUM_HEADS, HEAD_DIM)
            normed = rms_norm(hidden, gain_attn)
            query = apply_rope(jnp.dot(normed, q_weight, preferred_element_type=jnp.float32).reshape(head_shape), cosine, sine).astype(jnp.bfloat16)
            key_new = apply_rope(jnp.dot(normed, k_weight, preferred_element_type=jnp.float32).reshape(head_shape), cosine, sine).astype(jnp.bfloat16)
            val_new = jnp.dot(normed, v_weight, preferred_element_type=jnp.float32).astype(jnp.bfloat16).reshape(head_shape)
            keys_all = jnp.concatenate([key_pre, key_new], axis=0)
            vals_all = jnp.concatenate([val_pre, val_new], axis=0)
            scores = jnp.einsum('thd,nhd->htn', query.astype(jnp.float32), keys_all.astype(jnp.float32)) * scale
            scores = jnp.where(visible[None, :, :], scores, -1e30)
            attn_prob = jax.nn.softmax(scores, axis=-1).astype(jnp.bfloat16)
            mixed = jnp.einsum('htn,nhd->thd', attn_prob.astype(jnp.float32), vals_all.astype(jnp.float32))
            attn_out = mixed.astype(jnp.bfloat16).reshape(TOKENS, ATTN_WIDTH)
            hidden = (hidden.astype(jnp.float32) + jnp.dot(attn_out, o_weight, preferred_element_type=jnp.float32)).astype(jnp.bfloat16)
            normed_mlp = rms_norm(hidden, gain_mlp)
            gate = jnp.dot(normed_mlp, gate_weight, preferred_element_type=jnp.float32)
            upper = jnp.dot(normed_mlp, up_weight, preferred_element_type=jnp.float32)
            inner = (jax.nn.silu(gate) * upper).astype(jnp.bfloat16)
            hidden = (hidden.astype(jnp.float32) + jnp.dot(inner, down_weight, preferred_element_type=jnp.float32)).astype(jnp.bfloat16)
            return hidden, None

        out_rows, _ = lax.scan(layer_step, tok_rows, layer_stack)
        return out_rows

    return lax.map(one_request, (tok_hidden, page_idx))
```

```python
import functools
import jax
import jax.numpy as jnp
from jax import lax
from jax.experimental import pallas as pl
from jax.experimental.pallas import tpu as pltpu
from jax.sharding import PartitionSpec as P

NORM_EPS = 1e-6
ROPE_BASE = 10000.0
CHUNKS = 4
F32 = jnp.float32
BF16 = jnp.bfloat16


def rope_tables(offset, tokens, head_dim):
    positions = (offset + jnp.arange(tokens)).astype(F32)
    exponent = jnp.arange(head_dim // 2).astype(F32) * (-2.0 / head_dim)
    inv_freq = jnp.power(ROPE_BASE, exponent)
    angles = positions[:, None] * inv_freq[None, :]
    cosine, sine = jnp.cos(angles), jnp.sin(angles)
    return jnp.concatenate([cosine] * 4, axis=1), jnp.concatenate([-sine, sine] * 2, axis=1)


def rms_norm(vals, gain):
    vals_f = vals.astype(F32)
    inv_rms = lax.rsqrt(jnp.mean(vals_f * vals_f, axis=-1, keepdims=True) + NORM_EPS)
    return (vals_f * inv_rms * gain.astype(F32)).astype(BF16)


def pack_kernel(idx_ref, *refs):
    out_ref = refs[-1]
    pages = refs[:-1]
    page_len = pages[0].shape[4]
    pairs = out_ref.shape[2]
    for j, page in enumerate(pages):
        rows = pl.ds(j * page_len, page_len)
        for part in range(2):
            for i in range(pairs):
                both = jnp.concatenate([page[0, 0, part, 2 * i], page[0, 0, part, 2 * i + 1]], axis=-1)
                out_ref[0, part, i, rows, :] = both


def pack_pages(kv_heads, idx, layer):
    _, _, _, heads, page_len, dim = kv_heads.shape
    reqs, slots = idx.shape

    def page_spec(j):
        return pl.BlockSpec((1, 1, 2, heads, page_len, dim), lambda r, idx_ref: (layer, idx_ref[r, j], 0, 0, 0, 0))

    out_block = (1, 2, heads // 2, slots * page_len, 2 * dim)
    nbytes = kv_heads[0].size * 2
    return pl.pallas_call(
        pack_kernel,
        grid_spec=pltpu.PrefetchScalarGridSpec(
            num_scalar_prefetch=1,
            grid=(reqs,),
            in_specs=[page_spec(j) for j in range(slots)],
            out_specs=pl.BlockSpec(out_block, lambda r, idx_ref: (r, 0, 0, 0, 0)),
        ),
        out_shape=jax.ShapeDtypeStruct((reqs,) + out_block[1:], BF16),
        compiler_params=pltpu.CompilerParams(dimension_semantics=('arbitrary',)),
        cost_estimate=pl.CostEstimate(flops=0, bytes_accessed=3 * nbytes, transcendentals=0),
        name='pack_pages',
    )(idx, *([kv_heads] * slots))


def qkv_kernel(x_ref, gain_ref, cos_ref, sin_ref, wq_ref, wk_ref, wv_ref, q_ref, k_ref, v_ref, normed):
    @pl.when(pl.program_id(0) == 0)
    def _():
        normed[...] = rms_norm(x_ref[...], gain_ref[...])

    h = normed[...]
    lane = lax.broadcasted_iota(jnp.int32, cos_ref.shape, 1)
    low = (lane % 64) < 32
    cosine, sine = cos_ref[...], sin_ref[...]
    for w_ref, out_ref, rope in ((wq_ref, q_ref, True), (wk_ref, k_ref, True), (wv_ref, v_ref, False)):
        proj = jnp.dot(h, w_ref[0], preferred_element_type=F32)
        for i in range(out_ref.shape[0]):
            part = proj[:, i * 128:(i + 1) * 128]
            if rope:
                swapped = jnp.where(low, pltpu.roll(part, 96, 1), pltpu.roll(part, 32, 1))
                part = part * cosine + swapped * sine
            out_ref[i] = part.astype(BF16)


def qkv_proj(x, gain, cosine, sine, w_query, w_key, w_value, layer, tile=256):
    tokens, width = x.shape
    cols = w_query.shape[2]
    w_spec = pl.BlockSpec((1, width, tile), lambda n: (layer, 0, n))
    out_spec = pl.BlockSpec((tile // 128, tokens, 128), lambda n: (n, 0, 0))
    whole = lambda a: pl.BlockSpec(a.shape, lambda n: (0,) * a.ndim)
    out = jax.ShapeDtypeStruct((cols // 128, tokens, 128), BF16)
    return pl.pallas_call(
        qkv_kernel,
        grid=(cols // tile,),
        in_specs=[whole(x), whole(gain), whole(cosine), whole(sine), w_spec, w_spec, w_spec],
        out_specs=[out_spec] * 3,
        out_shape=[out] * 3,
        scratch_shapes=[pltpu.VMEM((tokens, width), BF16)],
        compiler_params=pltpu.CompilerParams(dimension_semantics=('arbitrary',)),
        cost_estimate=pl.CostEstimate(flops=6 * tokens * width * cols, bytes_accessed=6 * width * cols, transcendentals=0),
        name='qkv_proj',
    )(x, gain, cosine, sine, w_query, w_key, w_value)


def half_masks(shape, dtype):
    lane = lax.broadcasted_iota(jnp.int32, shape, 1)
    low = jnp.where(lane < 64, 1.0, 0.0)
    return low.astype(dtype), (1.0 - low).astype(dtype)


def block_diag(pair, low, high):
    return jnp.concatenate([pair * low, pair * high], axis=0)


def dot_t(a, b):
    return lax.dot_general(a, b, (((1,), (1,)), ((), ())), preferred_element_type=F32)


def attend_parts(query, parts, low_b, high_b, is_low, scale, masks):
    scores = []
    for (key, _), mask in zip(parts, masks):
        score = dot_t(query, block_diag(key, low_b, high_b)) * scale
        scores.append(score if mask is None else jnp.where(mask, score, -1e30))
    top0 = top1 = None
    for score in scores:
        a = jnp.max(jnp.where(is_low, score, -jnp.inf), axis=1, keepdims=True)
        b = jnp.max(jnp.where(is_low, -jnp.inf, score), axis=1, keepdims=True)
        top0 = a if top0 is None else jnp.maximum(top0, a)
        top1 = b if top1 is None else jnp.maximum(top1, b)
    top = jnp.where(is_low, top0, top1)
    sum0 = sum1 = out = None
    for score, (_, val) in zip(scores, parts):
        prob = jnp.exp(score - top)
        a = jnp.sum(jnp.where(is_low, prob, 0.0), axis=1, keepdims=True)
        b = jnp.sum(jnp.where(is_low, 0.0, prob), axis=1, keepdims=True)
        o = jnp.dot(prob.astype(BF16), block_diag(val, low_b, high_b), preferred_element_type=F32)
        sum0, sum1, out = (a, b, o) if out is None else (sum0 + a, sum1 + b, out + o)
    return out / jnp.where(is_low, sum0, sum1), (top0, top1, sum0, sum1)


def ring_kernel(group, scale, q_ref, k_ref, v_ref, kv_hbm, out_ref, kv, qbuf, obuf, loc, home, kv_sem, q_send, q_recv, o_send, o_recv):
    pairs, tokens, lanes = q_ref.shape
    half = pairs // 2
    rows = tokens // CHUNKS
    me = lax.axis_index('pool')
    right, left = lax.rem(me + 1, group), lax.rem(me + group - 1, group)
    toward = (right, left)

    barrier = pltpu.get_barrier_semaphore()
    for neighbour in toward:
        pl.semaphore_signal(barrier, inc=1, device_id={'pool': neighbour}, device_id_type=pl.DeviceIdType.MESH)
    pl.semaphore_wait(barrier, 2)

    def request_at(d, s):
        return lax.rem(me - s + group, group) if d == 0 else lax.rem(me + s, group)

    def kv_copy(d, s):
        return pltpu.make_async_copy(kv_hbm.at[request_at(d, s), :, pl.ds(half * d, half)], kv.at[d, s], kv_sem.at[d, s])

    def q_copy(d, s):
        return pltpu.make_async_remote_copy(
            src_ref=qbuf.at[d, s], dst_ref=qbuf.at[d, s + 1], send_sem=q_send.at[d, s], recv_sem=q_recv.at[d, s + 1],
            device_id={'pool': toward[d]}, device_id_type=pl.DeviceIdType.MESH)

    def q_first(d):
        return pltpu.make_async_remote_copy(
            src_ref=q_ref.at[pl.ds(half * d, half)], dst_ref=qbuf.at[d, 1], send_sem=q_send.at[d, 0], recv_sem=q_recv.at[d, 1],
            device_id={'pool': toward[d]}, device_id_type=pl.DeviceIdType.MESH)

    def o_copy(d, s, c):
        return pltpu.make_async_remote_copy(
            src_ref=obuf.at[d, s - 1, c], dst_ref=obuf.at[d, s, c], send_sem=o_send.at[d, s - 1, c], recv_sem=o_recv.at[d, s, c],
            device_id={'pool': toward[d]}, device_id_type=pl.DeviceIdType.MESH)

    for d in range(2):
        q_first(d).start()

    @pl.loop(0, group)
    def _(s):
        for d in range(2):
            kv_copy(d, s).start()

    lane = lax.broadcasted_iota(jnp.int32, (tokens, lanes), 1)
    is_low = lane < 64
    low_b, high_b = half_masks((tokens, lanes), BF16)

    def put(stat, value0, value1, j):
        return jnp.where(lane == j, value0, jnp.where(lane == 64 + j, value1, stat))

    def local_part(d, s, dest, query_at, extra):
        def one(j, carry):
            tops, sums = carry
            parts = [(kv[d, s, 0, j], kv[d, s, 1, j])] + extra[0](j)
            out, (top0, top1, sum0, sum1) = attend_parts(query_at(j), parts, low_b, high_b, is_low, scale, [None] + extra[1])
            for c in range(CHUNKS):
                dest[d, c, j] = out[c * rows:(c + 1) * rows]
            return put(tops, top0, top1, j), put(sums, sum0, sum1, j)

        zero = jnp.zeros((tokens, lanes), F32)
        tops, sums = lax.fori_loop(0, half, one, (zero, zero + 1.0), unroll=3)
        stat = tops + jnp.log(sums)
        for c in range(CHUNKS):
            dest[d, c, half] = stat[c * rows:(c + 1) * rows]

    key_at = lax.rem(lane, 64)
    causal = key_at <= lax.broadcasted_iota(jnp.int32, (tokens, lanes), 0)
    for d in range(2):
        kv_copy(d, 0).wait()
        local_part(d, 0, home, lambda j, d=d: q_ref[half * d + j],
                   (lambda j, d=d: [(k_ref[half * d + j], v_ref[half * d + j])], [causal]))

    row_low = lax.broadcasted_iota(jnp.int32, (rows, lanes), 1) < 64

    def weights(far, near):
        gap = far - near
        joint = jnp.maximum(far, near) + jnp.log(1.0 + jnp.exp(-jnp.abs(gap)))
        return 1.0 / (1.0 + jnp.exp(-gap)), joint

    def spread(stat, j):
        return jnp.where(row_low, stat[:, j:j + 1], stat[:, 64 + j:65 + j])

    def step(s, _):
        for d in range(2):
            q_copy(d, s - 1).wait_recv()

            @pl.when(s < group - 1)
            def _():
                q_copy(d, s).start()

        for d in range(2):
            kv_copy(d, s).wait()
            local_part(d, s, loc, lambda j, d=d: qbuf[d, s, j], (lambda j: [], []))

        @pl.when(s == 1)
        def _():
            for d in range(2):
                for c in range(CHUNKS):
                    obuf[d, 1, c] = loc[d, c]

        for c in range(CHUNKS):
            for d in range(2):
                @pl.when(s > 1)
                def _():
                    o_copy(d, s, c).wait_recv()
                    weight, joint = weights(obuf[d, s, c, half], loc[d, c, half])
                    for j in range(half):
                        near = loc[d, c, j]
                        obuf[d, s, c, j] = near + spread(weight, j) * (obuf[d, s, c, j] - near)
                    obuf[d, s, c, half] = joint

                o_copy(d, s + 1, c).start()
        return 0

    lax.fori_loop(1, group, step, 0)

    for c in range(CHUNKS):
        for d in range(2):
            o_copy(d, group, c).wait_recv()
            weight, _ = weights(obuf[d, group, c, half], home[d, c, half])
            for j in range(half):
                near = home[d, c, j]
                out_ref[half * d + j, c * rows:(c + 1) * rows, :] = (near + spread(weight, j) * (obuf[d, group, c, j] - near)).astype(BF16)

    for d in range(2):
        q_first(d).wait_send()

    @pl.loop(1, group)
    def _(s):
        for d in range(2):
            @pl.when(s < group - 1)
            def _():
                q_copy(d, s).wait_send()

            for c in range(CHUNKS):
                o_copy(d, s + 1, c).wait_send()


def ring_attention(query, key, val, packed, group, scale):
    pairs, tokens, lanes = query.shape
    half = pairs // 2
    rows = tokens // CHUNKS
    sem = pltpu.SemaphoreType.DMA
    vmem = pl.BlockSpec(memory_space=pltpu.VMEM)
    scratch = [
        pltpu.VMEM((2, group, 2, half, tokens, lanes), BF16),
        pltpu.VMEM((2, group, half, tokens, lanes), BF16),
        pltpu.VMEM((2, group + 1, CHUNKS, half + 1, rows, lanes), F32),
        pltpu.VMEM((2, CHUNKS, half + 1, rows, lanes), F32),
        pltpu.VMEM((2, CHUNKS, half + 1, rows, lanes), F32),
        sem((2, group)),
        sem((2, group)),
        sem((2, group)),
        sem((2, group + 1, CHUNKS)),
        sem((2, group + 1, CHUNKS)),
    ]
    return pl.pallas_call(
        functools.partial(ring_kernel, group, scale),
        out_shape=jax.ShapeDtypeStruct(query.shape, BF16),
        in_specs=[vmem, vmem, vmem, pl.BlockSpec(memory_space=pl.ANY)],
        out_specs=vmem,
        scratch_shapes=scratch,
        compiler_params=pltpu.CompilerParams(collective_id=0, has_side_effects=True),
        name='ring_attention',
    )(query, key, val, packed)


def out_kernel(x_ref, a_ref, w_ref, out_ref, rowwise):
    @pl.when(pl.program_id(0) == 0)
    def _():
        for i in range(a_ref.shape[0]):
            rowwise[:, i * 128:(i + 1) * 128] = a_ref[i]

    proj = jnp.dot(rowwise[...], w_ref[0], preferred_element_type=F32)
    out_ref[...] = (x_ref[...].astype(F32) + proj).astype(BF16)


def out_proj(x, mixed, w_out, layer, tile=256):
    tokens, width = x.shape
    depth = w_out.shape[1]
    x_spec = pl.BlockSpec((tokens, tile), lambda n: (0, n))
    return pl.pallas_call(
        out_kernel,
        grid=(width // tile,),
        in_specs=[x_spec, pl.BlockSpec(mixed.shape, lambda n: (0, 0, 0)), pl.BlockSpec((1, depth, tile), lambda n: (layer, 0, n))],
        out_specs=x_spec,
        out_shape=jax.ShapeDtypeStruct(x.shape, BF16),
        scratch_shapes=[pltpu.VMEM((tokens, depth), BF16)],
        compiler_params=pltpu.CompilerParams(dimension_semantics=('arbitrary',)),
        cost_estimate=pl.CostEstimate(flops=2 * tokens * width * depth, bytes_accessed=2 * width * depth, transcendentals=0),
        name='out_proj',
    )(x, mixed, w_out)


def mlp_kernel(x_ref, gain_ref, wg_ref, wu_ref, wd_ref, out_ref, normed, total):
    step = pl.program_id(0)

    @pl.when(step == 0)
    def _():
        normed[...] = rms_norm(x_ref[...], gain_ref[...])
        total[...] = jnp.zeros_like(total)

    h = normed[...]
    gate = jnp.dot(h, wg_ref[0], preferred_element_type=F32)
    upper = jnp.dot(h, wu_ref[0], preferred_element_type=F32)
    inner = (jax.nn.silu(gate) * upper).astype(BF16)
    total[...] += jnp.dot(inner, wd_ref[0], preferred_element_type=F32)

    @pl.when(step == pl.num_programs(0) - 1)
    def _():
        out_ref[...] = (x_ref[...].astype(F32) + total[...]).astype(BF16)


def mlp(x, gain, w_gate, w_up, w_down, layer, tile=384):
    tokens, width = x.shape
    inner = w_gate.shape[2]
    in_spec = pl.BlockSpec((1, width, tile), lambda n: (layer, 0, n))
    whole = lambda a: pl.BlockSpec(a.shape, lambda n: (0,) * a.ndim)
    return pl.pallas_call(
        mlp_kernel,
        grid=(inner // tile,),
        in_specs=[whole(x), whole(gain), in_spec, in_spec, pl.BlockSpec((1, tile, width), lambda n: (layer, n, 0))],
        out_specs=whole(x),
        out_shape=jax.ShapeDtypeStruct(x.shape, BF16),
        scratch_shapes=[pltpu.VMEM((tokens, width), BF16), pltpu.VMEM((tokens, width), F32)],
        compiler_params=pltpu.CompilerParams(dimension_semantics=('arbitrary',)),
        cost_estimate=pl.CostEstimate(flops=6 * tokens * width * inner, bytes_accessed=6 * width * inner, transcendentals=tokens * inner),
        name='mlp',
    )(x, gain, w_gate, w_up, w_down)


def solution(mesh):
    group = mesh.shape['pool']

    def local_program(kv_local, idx_local, hid_local, attn_norm, w_query, w_key, w_value, w_out, mlp_norm, w_gate, w_up, w_down):
        layers, _, _, page_len, _, dim = kv_local.shape
        prefix = group * idx_local.shape[2] * page_len
        cosine, sine = rope_tables(prefix, hid_local.shape[1], dim)
        idx = idx_local[:, 0, :]
        kv_heads = jnp.transpose(kv_local, (0, 1, 2, 4, 3, 5))
        x = hid_local[0]
        for layer in range(layers):
            packed = pack_pages(kv_heads, idx, layer)
            query, key, val = qkv_proj(x, attn_norm[layer:layer + 1], cosine, sine, w_query, w_key, w_value, layer)
            mixed = ring_attention(query, key, val, packed, group, dim ** -0.5)
            x = out_proj(x, mixed, w_out, layer)
            x = mlp(x, mlp_norm[layer:layer + 1], w_gate, w_up, w_down, layer)
        return x[None]

    data_specs = (P(None, ('rep', 'pool')), P(None, ('rep', 'pool'), None), P(('rep', 'pool')))
    return jax.shard_map(local_program, mesh=mesh, in_specs=data_specs + (P(),) * 9, out_specs=P(('rep', 'pool')), check_vma=False)
```

```python
import functools
import jax
import jax.numpy as jnp
from jax import lax
from jax.experimental import pallas as pl
from jax.experimental.pallas import tpu as pltpu
from jax.sharding import PartitionSpec as P

NORM_EPS = 1e-6
ROPE_BASE = 10000.0
CHUNKS = 4
F32 = jnp.float32
BF16 = jnp.bfloat16


def rope_tables(offset, tokens, head_dim):
    positions = (offset + jnp.arange(tokens)).astype(F32)
    exponent = jnp.arange(head_dim // 2).astype(F32) * (-2.0 / head_dim)
    inv_freq = jnp.power(ROPE_BASE, exponent)
    angles = positions[:, None] * inv_freq[None, :]
    cosine, sine = jnp.cos(angles), jnp.sin(angles)
    return jnp.concatenate([cosine] * 4, axis=1), jnp.concatenate([-sine, sine] * 2, axis=1)


def rms_norm(vals, gain):
    vals_f = vals.astype(F32)
    inv_rms = lax.rsqrt(jnp.mean(vals_f * vals_f, axis=-1, keepdims=True) + NORM_EPS)
    return (vals_f * inv_rms * gain.astype(F32)).astype(BF16)


def pack_kernel(layer, idx_ref, kv_hbm, out_ref, pages, sems):
    depth, slots = pages.shape[0], pages.shape[1]
    page_len = pages.shape[4]
    pairs = out_ref.shape[2]
    req, reqs = pl.program_id(0), pl.num_programs(0)

    def read(r, j):
        slot = lax.rem(r, depth)
        return pltpu.make_async_copy(kv_hbm.at[layer, idx_ref[r, j]], pages.at[slot, j], sems.at[slot, j])

    @pl.when(req == 0)
    def _():
        for r in range(depth - 1):
            for j in range(slots):
                read(r, j).start()

    @pl.when(req + depth - 1 < reqs)
    def _():
        for j in range(slots):
            read(req + depth - 1, j).start()

    slot = lax.rem(req, depth)
    for j in range(slots):
        read(req, j).wait()
        rows = pl.ds(j * page_len, page_len)
        for part in range(2):
            for i in range(pairs):
                both = jnp.concatenate([pages[slot, j, part, 2 * i], pages[slot, j, part, 2 * i + 1]], axis=-1)
                out_ref[0, part, i, rows, :] = both


def pack_pages(kv_heads, idx, layer, depth=4):
    _, _, _, heads, page_len, dim = kv_heads.shape
    reqs, slots = idx.shape
    out_block = (1, 2, heads // 2, slots * page_len, 2 * dim)
    nbytes = kv_heads[0].size * 2
    return pl.pallas_call(
        functools.partial(pack_kernel, layer),
        grid=(reqs,),
        in_specs=[pl.BlockSpec(memory_space=pltpu.SMEM), pl.BlockSpec(memory_space=pl.ANY)],
        out_specs=pl.BlockSpec(out_block, lambda r: (r, 0, 0, 0, 0)),
        out_shape=jax.ShapeDtypeStruct((reqs,) + out_block[1:], BF16),
        scratch_shapes=[
            pltpu.VMEM((depth, slots, 2, heads, page_len, dim), BF16),
            pltpu.SemaphoreType.DMA((depth, slots)),
        ],
        compiler_params=pltpu.CompilerParams(dimension_semantics=('arbitrary',)),
        cost_estimate=pl.CostEstimate(flops=0, bytes_accessed=3 * nbytes, transcendentals=0),
        name='pack_pages',
    )(idx, kv_heads)


def qkv_kernel(layer, x_ref, gain_ref, cos_ref, sin_ref, wq_hbm, wk_hbm, wv_hbm, q_ref, k_ref, v_ref, normed, slab, sems):
    depth, tile = slab.shape[0], slab.shape[3]
    tiles = wq_hbm.shape[2] // tile
    weights = (wq_hbm, wk_hbm, wv_hbm)

    def read(t, i):
        slot = lax.rem(t, depth)
        cols = pl.ds(pl.multiple_of(t * tile, tile), tile)
        return pltpu.make_async_copy(weights[i].at[layer, :, cols], slab.at[slot, i], sems.at[slot, i])

    for t in range(depth):
        for i in range(3):
            read(t, i).start()

    normed[...] = rms_norm(x_ref[...], gain_ref[...])
    lane = lax.broadcasted_iota(jnp.int32, cos_ref.shape, 1)
    low = (lane % 64) < 32

    def one(t, _):
        slot = lax.rem(t, depth)
        for i, out_ref in enumerate((q_ref, k_ref, v_ref)):
            read(t, i).wait()
            proj = jnp.dot(normed[...], slab[slot, i], preferred_element_type=F32)
            for p in range(tile // 128):
                part = proj[:, p * 128:(p + 1) * 128]
                if i < 2:
                    swapped = jnp.where(low, pltpu.roll(part, 96, 1), pltpu.roll(part, 32, 1))
                    part = part * cos_ref[...] + swapped * sin_ref[...]
                out_ref[t * (tile // 128) + p] = part.astype(BF16)

        @pl.when(t + depth < tiles)
        def _():
            for i in range(3):
                read(t + depth, i).start()

        return 0

    lax.fori_loop(0, tiles, one, 0)


def qkv_proj(x, gain, cosine, sine, w_query, w_key, w_value, layer, tile=256, depth=4):
    tokens, width = x.shape
    cols = w_query.shape[2]
    vmem, hbm = pl.BlockSpec(memory_space=pltpu.VMEM), pl.BlockSpec(memory_space=pl.ANY)
    out = jax.ShapeDtypeStruct((cols // 128, tokens, 128), BF16)
    return pl.pallas_call(
        functools.partial(qkv_kernel, layer),
        in_specs=[vmem] * 4 + [hbm] * 3,
        out_specs=[vmem] * 3,
        out_shape=[out] * 3,
        scratch_shapes=[
            pltpu.VMEM((tokens, width), BF16),
            pltpu.VMEM((depth, 3, width, tile), BF16),
            pltpu.SemaphoreType.DMA((depth, 3)),
        ],
        cost_estimate=pl.CostEstimate(flops=6 * tokens * width * cols, bytes_accessed=6 * width * cols, transcendentals=0),
        name='qkv_proj',
    )(x, gain, cosine, sine, w_query, w_key, w_value)


def half_masks(shape, dtype):
    lane = lax.broadcasted_iota(jnp.int32, shape, 1)
    low = jnp.where(lane < 64, 1.0, 0.0)
    return low.astype(dtype), (1.0 - low).astype(dtype)


def block_diag(pair, low, high):
    return jnp.concatenate([pair * low, pair * high], axis=0)


def dot_t(a, b):
    return lax.dot_general(a, b, (((1,), (1,)), ((), ())), preferred_element_type=F32)


def layer_kernel(layer, group, scale, q_ref, k_ref, v_ref, x_ref, gain_ref, kv_hbm, wo_hbm, wg_hbm, wu_hbm, wd_hbm, out_ref,
                 kv, qbuf, obuf, loc, home, score, prob, rowwise, normed, total, wo, slab_in, slab_out,
                 kv_sem, q_send, q_recv, o_send, o_recv, wo_sem, sems):
    pairs, tokens, lanes = q_ref.shape
    half = pairs // 2
    rows = tokens // CHUNKS
    me = lax.axis_index('pool')
    right, left = lax.rem(me + 1, group), lax.rem(me + group - 1, group)
    toward = (right, left)

    barrier = pltpu.get_barrier_semaphore()
    for neighbour in toward:
        pl.semaphore_signal(barrier, inc=1, device_id={'pool': neighbour}, device_id_type=pl.DeviceIdType.MESH)
    pl.semaphore_wait(barrier, 2)

    def request_at(d, s):
        return lax.rem(me - s + group, group) if d == 0 else lax.rem(me + s, group)

    def kv_copy(d, s):
        return pltpu.make_async_copy(kv_hbm.at[request_at(d, s), :, pl.ds(half * d, half)], kv.at[d, s], kv_sem.at[d, s])

    def q_copy(d, s):
        return pltpu.make_async_remote_copy(
            src_ref=qbuf.at[d, s], dst_ref=qbuf.at[d, s + 1], send_sem=q_send.at[d, s], recv_sem=q_recv.at[d, s + 1],
            device_id={'pool': toward[d]}, device_id_type=pl.DeviceIdType.MESH)

    def q_first(d):
        return pltpu.make_async_remote_copy(
            src_ref=q_ref.at[pl.ds(half * d, half)], dst_ref=qbuf.at[d, 1], send_sem=q_send.at[d, 0], recv_sem=q_recv.at[d, 1],
            device_id={'pool': toward[d]}, device_id_type=pl.DeviceIdType.MESH)

    def o_copy(d, s, c):
        return pltpu.make_async_remote_copy(
            src_ref=obuf.at[d, s - 1, c], dst_ref=obuf.at[d, s, c], send_sem=o_send.at[d, s - 1, c], recv_sem=o_recv.at[d, s, c],
            device_id={'pool': toward[d]}, device_id_type=pl.DeviceIdType.MESH)

    for d in range(2):
        q_first(d).start()

    @pl.loop(0, group)
    def _(s):
        for d in range(2):
            kv_copy(d, s).start()

    depth, tile = slab_out.shape[0], slab_out.shape[1]
    tiles = wg_hbm.shape[2] // tile
    wo_tiles, wo_tile = wo.shape[0], wo.shape[2]

    def read_out(t):
        return pltpu.make_async_copy(wo_hbm.at[layer, :, pl.ds(t * wo_tile, wo_tile)], wo.at[t], wo_sem.at[t])

    def reads(t):
        slot = lax.rem(t, depth)
        cols = pl.ds(pl.multiple_of(t * tile, tile), tile)
        return (pltpu.make_async_copy(wg_hbm.at[layer, :, cols], slab_in.at[slot, 0], sems.at[slot, 0]),
                pltpu.make_async_copy(wu_hbm.at[layer, :, cols], slab_in.at[slot, 1], sems.at[slot, 1]),
                pltpu.make_async_copy(wd_hbm.at[layer, cols, :], slab_out.at[slot], sems.at[slot, 2]))

    for t in range(wo_tiles):
        read_out(t).start()
    for t in range(depth):
        for copy in reads(t):
            copy.start()

    low_b, high_b = half_masks((tokens, lanes), BF16)

    row_lane = lax.broadcasted_iota(jnp.int32, (rows, lanes), 1)
    row_low = row_lane < 64
    row_at = lax.broadcasted_iota(jnp.int32, (rows, lanes), 0)

    def local_part(d, dest, query_at, key_at, val_at, causal):
        for j in range(half):
            score[d, j] = dot_t(query_at(j), block_diag(key_at(j), low_b, high_b)) * scale
        for c in range(CHUNKS):
            here = slice(c * rows, (c + 1) * rows)
            tops = jnp.zeros((rows, lanes), F32)
            sums = jnp.ones((rows, lanes), F32)
            for j in range(half):
                part = score[d, j, here]
                if causal:
                    part = jnp.where(lax.rem(row_lane, 64) <= row_at + c * rows, part, -1e30)
                top0 = jnp.max(jnp.where(row_low, part, -jnp.inf), axis=1, keepdims=True)
                top1 = jnp.max(jnp.where(row_low, -jnp.inf, part), axis=1, keepdims=True)
                raised = jnp.exp(part - jnp.where(row_low, top0, top1))
                sum0 = jnp.sum(jnp.where(row_low, raised, 0.0), axis=1, keepdims=True)
                sum1 = jnp.sum(jnp.where(row_low, 0.0, raised), axis=1, keepdims=True)
                prob[d, j, here] = (raised * (1.0 / jnp.where(row_low, sum0, sum1))).astype(BF16)
                at0, at1 = row_lane == j, row_lane == 64 + j
                tops = jnp.where(at0, top0, jnp.where(at1, top1, tops))
                sums = jnp.where(at0, sum0, jnp.where(at1, sum1, sums))
            dest[d, c, half] = tops + jnp.log(sums)
        for j in range(half):
            out = jnp.dot(prob[d, j], block_diag(val_at(j), low_b, high_b), preferred_element_type=F32)
            for c in range(CHUNKS):
                dest[d, c, j] = out[c * rows:(c + 1) * rows]

    def weights(far, near):
        gap = far - near
        joint = jnp.maximum(far, near) + jnp.log(1.0 + jnp.exp(-jnp.abs(gap)))
        return 1.0 / (1.0 + jnp.exp(-gap)), joint

    def spread(stat, j):
        return jnp.where(row_low, stat[:, j:j + 1], stat[:, 64 + j:65 + j])

    def merge(d, c, far, near):
        weight, joint = weights(far[half], near[half])
        outs = [near[j] + spread(weight, j) * (far[j] - near[j]) for j in range(half)]
        return outs, joint

    for d in range(2):
        kv_copy(d, 0).wait()
        own = half * d
        local_part(d, home, lambda j: q_ref[own + j], lambda j: kv[d, 0, 0, j], lambda j: kv[d, 0, 1, j], False)
        local_part(d, loc, lambda j: q_ref[own + j], lambda j: k_ref[own + j], lambda j: v_ref[own + j], True)
        for c in range(CHUNKS):
            outs, joint = merge(d, c, home.at[d, c], loc.at[d, c])
            for j in range(half):
                home[d, c, j] = outs[j]
            home[d, c, half] = joint

    def step(s, _):
        for d in range(2):
            q_copy(d, s - 1).wait_recv()

            @pl.when(s < group - 1)
            def _():
                q_copy(d, s).start()

        for d in range(2):
            kv_copy(d, s).wait()
            local_part(d, loc, lambda j: qbuf[d, s, j], lambda j: kv[d, s, 0, j], lambda j: kv[d, s, 1, j], False)

        @pl.when(s == 1)
        def _():
            for d in range(2):
                for c in range(CHUNKS):
                    obuf[d, 1, c] = loc[d, c]

        for c in range(CHUNKS):
            for d in range(2):
                @pl.when(s > 1)
                def _():
                    o_copy(d, s, c).wait_recv()
                    outs, joint = merge(d, c, obuf.at[d, s, c], loc.at[d, c])
                    for j in range(half):
                        obuf[d, s, c, j] = outs[j]
                    obuf[d, s, c, half] = joint

                o_copy(d, s + 1, c).start()
        return 0

    lax.fori_loop(1, group, step, 0)

    for c in range(CHUNKS):
        for d in range(2):
            o_copy(d, group, c).wait_recv()
            outs, _ = merge(d, c, obuf.at[d, group, c], home.at[d, c])
            for j in range(half):
                at = (half * d + j) * lanes
                rowwise[c * rows:(c + 1) * rows, at:at + lanes] = outs[j].astype(BF16)

    for t in range(wo_tiles):
        read_out(t).wait()
        cols = slice(t * wo_tile, (t + 1) * wo_tile)
        proj = jnp.dot(rowwise[...], wo[t], preferred_element_type=F32)
        out_ref[:, cols] = (x_ref[:, cols].astype(F32) + proj).astype(BF16)
    normed[...] = rms_norm(out_ref[...], gain_ref[...])
    total[...] = jnp.zeros_like(total)

    def one(t, _):
        slot = lax.rem(t, depth)
        gate_read, up_read, down_read = reads(t)
        gate_read.wait()
        gate = jnp.dot(normed[...], slab_in[slot, 0], preferred_element_type=F32)
        up_read.wait()
        upper = jnp.dot(normed[...], slab_in[slot, 1], preferred_element_type=F32)
        inner = (jax.nn.silu(gate) * upper).astype(BF16)
        down_read.wait()
        total[...] += jnp.dot(inner, slab_out[slot], preferred_element_type=F32)

        @pl.when(t + depth < tiles)
        def _():
            for copy in reads(t + depth):
                copy.start()

        return 0

    lax.fori_loop(0, tiles, one, 0)
    out_ref[...] = (out_ref[...].astype(F32) + total[...]).astype(BF16)

    for d in range(2):
        q_first(d).wait_send()

    @pl.loop(1, group)
    def _(s):
        for d in range(2):
            @pl.when(s < group - 1)
            def _():
                q_copy(d, s).wait_send()

            for c in range(CHUNKS):
                o_copy(d, s + 1, c).wait_send()


def layer_rest(x, query, key, val, packed, gain, w_out, w_gate, w_up, w_down, layer, group, scale, tile=384, depth=4, wo_tile=768):
    pairs, tokens, lanes = query.shape
    width, attn, inner = x.shape[1], w_out.shape[1], w_gate.shape[2]
    half = pairs // 2
    rows = tokens // CHUNKS
    sem = pltpu.SemaphoreType.DMA
    vmem, hbm = pl.BlockSpec(memory_space=pltpu.VMEM), pl.BlockSpec(memory_space=pl.ANY)
    scratch = [
        pltpu.VMEM((2, group, 2, half, tokens, lanes), BF16),
        pltpu.VMEM((2, group, half, tokens, lanes), BF16),
        pltpu.VMEM((2, group + 1, CHUNKS, half + 1, rows, lanes), F32),
        pltpu.VMEM((2, CHUNKS, half + 1, rows, lanes), F32),
        pltpu.VMEM((2, CHUNKS, half + 1, rows, lanes), F32),
        pltpu.VMEM((2, half, tokens, lanes), F32),
        pltpu.VMEM((2, half, tokens, lanes), BF16),
        pltpu.VMEM((tokens, attn), BF16),
        pltpu.VMEM((tokens, width), BF16),
        pltpu.VMEM((tokens, width), F32),
        pltpu.VMEM((width // wo_tile, attn, wo_tile), BF16),
        pltpu.VMEM((depth, 2, width, tile), BF16),
        pltpu.VMEM((depth, tile, width), BF16),
        sem((2, group)),
        sem((2, group)),
        sem((2, group)),
        sem((2, group + 1, CHUNKS)),
        sem((2, group + 1, CHUNKS)),
        sem((width // wo_tile,)),
        sem((depth, 3)),
    ]
    return pl.pallas_call(
        functools.partial(layer_kernel, layer, group, scale),
        out_shape=jax.ShapeDtypeStruct(x.shape, BF16),
        in_specs=[vmem] * 5 + [hbm] * 5,
        out_specs=vmem,
        scratch_shapes=scratch,
        compiler_params=pltpu.CompilerParams(collective_id=layer, has_side_effects=True, vmem_limit_bytes=67_000_000),
        name='layer_rest',
    )(query, key, val, x, gain, packed, w_out, w_gate, w_up, w_down)


def solution(mesh):
    group = mesh.shape['pool']

    def local_program(kv_local, idx_local, hid_local, attn_norm, w_query, w_key, w_value, w_out, mlp_norm, w_gate, w_up, w_down):
        layers, _, _, page_len, _, dim = kv_local.shape
        prefix = group * idx_local.shape[2] * page_len
        cosine, sine = rope_tables(prefix, hid_local.shape[1], dim)
        idx = idx_local[:, 0, :]
        kv_heads = jnp.transpose(kv_local, (0, 1, 2, 4, 3, 5))
        x = hid_local[0]
        for layer in range(layers):
            packed = pack_pages(kv_heads, idx, layer)
            query, key, val = qkv_proj(x, attn_norm[layer:layer + 1], cosine, sine, w_query, w_key, w_value, layer)
            x = layer_rest(x, query, key, val, packed, mlp_norm[layer:layer + 1], w_out, w_gate, w_up, w_down, layer, group, dim ** -0.5)
        return x[None]

    data_specs = (P(None, ('rep', 'pool')), P(None, ('rep', 'pool'), None), P(('rep', 'pool')))
    return jax.shard_map(local_program, mesh=mesh, in_specs=data_specs + (P(),) * 9, out_specs=P(('rep', 'pool')), check_vma=False)
```

```python
import functools
import jax
import jax.numpy as jnp
from jax import lax
from jax.experimental import pallas as pl
from jax.experimental.pallas import tpu as pltpu
from jax.sharding import PartitionSpec as P

NORM_EPS = 1e-6
ROPE_BASE = 10000.0
CHUNKS = 4
F32 = jnp.float32
BF16 = jnp.bfloat16


def rope_tables(offset, tokens, head_dim):
    positions = (offset + jnp.arange(tokens)).astype(F32)
    exponent = jnp.arange(head_dim // 2).astype(F32) * (-2.0 / head_dim)
    inv_freq = jnp.power(ROPE_BASE, exponent)
    angles = positions[:, None] * inv_freq[None, :]
    cosine, sine = jnp.cos(angles), jnp.sin(angles)
    return jnp.concatenate([cosine] * 4, axis=1), jnp.concatenate([-sine, sine] * 2, axis=1)


def rms_norm(vals, gain):
    vals_f = vals.astype(F32)
    inv_rms = lax.rsqrt(jnp.mean(vals_f * vals_f, axis=-1, keepdims=True) + NORM_EPS)
    return (vals_f * inv_rms * gain.astype(F32)).astype(BF16)


def front_kernel(layer, idx_ref, x_ref, gain_ref, cos_ref, sin_ref, wq_hbm, wk_hbm, wv_hbm, kv_hbm,
                 q_ref, k_ref, v_ref, packed_hbm, normed, slab, pages, block, sems, page_sems, out_sems):
    depth, tile = slab.shape[0], slab.shape[3]
    tiles = wq_hbm.shape[2] // tile
    weights = (wq_hbm, wk_hbm, wv_hbm)
    ahead, slots, page_len = pages.shape[0], pages.shape[1], pages.shape[4]
    reqs, pairs = idx_ref.shape[0], block.shape[2]

    def read(t, i):
        slot = lax.rem(t, depth)
        cols = pl.ds(pl.multiple_of(t * tile, tile), tile)
        return pltpu.make_async_copy(weights[i].at[layer, :, cols], slab.at[slot, i], sems.at[slot, i])

    def read_page(r, j):
        slot = lax.rem(r, ahead)
        return pltpu.make_async_copy(kv_hbm.at[layer, idx_ref[r, j]], pages.at[slot, j], page_sems.at[slot, j])

    def write(r):
        slot = lax.rem(r, 2)
        return pltpu.make_async_copy(block.at[slot], packed_hbm.at[r], out_sems.at[slot])

    for t in range(depth):
        for i in range(3):
            read(t, i).start()
    for r in range(ahead):
        for j in range(slots):
            read_page(r, j).start()

    normed[...] = rms_norm(x_ref[...], gain_ref[...])
    lane = lax.broadcasted_iota(jnp.int32, cos_ref.shape, 1)
    low = (lane % 64) < 32

    def project(t, _):
        slot = lax.rem(t, depth)
        for i, out_ref in enumerate((q_ref, k_ref, v_ref)):
            read(t, i).wait()
            proj = jnp.dot(normed[...], slab[slot, i], preferred_element_type=F32)
            for p in range(tile // 128):
                part = proj[:, p * 128:(p + 1) * 128]
                if i < 2:
                    swapped = jnp.where(low, pltpu.roll(part, 96, 1), pltpu.roll(part, 32, 1))
                    part = part * cos_ref[...] + swapped * sin_ref[...]
                out_ref[t * (tile // 128) + p] = part.astype(BF16)

            @pl.when(t + depth < tiles)
            def _():
                read(t + depth, i).start()

        return 0

    lax.fori_loop(0, tiles, project, 0)

    def pack(r, _):
        slot, out_slot = lax.rem(r, ahead), lax.rem(r, 2)

        @pl.when(r >= 2)
        def _():
            write(r - 2).wait()

        for j in range(slots):
            read_page(r, j).wait()
            rows = pl.ds(j * page_len, page_len)
            for part in range(2):
                for i in range(pairs):
                    both = jnp.concatenate([pages[slot, j, part, 2 * i], pages[slot, j, part, 2 * i + 1]], axis=-1)
                    block[out_slot, part, i, rows, :] = both
        write(r).start()

        @pl.when(r + ahead < reqs)
        def _():
            for j in range(slots):
                read_page(r + ahead, j).start()

        return 0

    lax.fori_loop(0, reqs, pack, 0)
    for r in (reqs - 2, reqs - 1):
        write(r).wait()


def layer_front(x, idx, gain, cosine, sine, w_query, w_key, w_value, kv_heads, layer, tile=256, depth=4, ahead=8):
    tokens, width = x.shape
    cols = w_query.shape[2]
    _, _, _, heads, page_len, dim = kv_heads.shape
    reqs, slots = idx.shape
    block = (2, heads // 2, slots * page_len, 2 * dim)
    vmem, hbm = pl.BlockSpec(memory_space=pltpu.VMEM), pl.BlockSpec(memory_space=pl.ANY)
    out = jax.ShapeDtypeStruct((cols // 128, tokens, 128), BF16)
    return pl.pallas_call(
        functools.partial(front_kernel, layer),
        in_specs=[pl.BlockSpec(memory_space=pltpu.SMEM)] + [vmem] * 4 + [hbm] * 4,
        out_specs=[vmem] * 3 + [hbm],
        out_shape=[out] * 3 + [jax.ShapeDtypeStruct((reqs,) + block, BF16)],
        scratch_shapes=[
            pltpu.VMEM((tokens, width), BF16),
            pltpu.VMEM((depth, 3, width, tile), BF16),
            pltpu.VMEM((ahead, slots, 2, heads, page_len, dim), BF16),
            pltpu.VMEM((2,) + block, BF16),
            pltpu.SemaphoreType.DMA((depth, 3)),
            pltpu.SemaphoreType.DMA((ahead, slots)),
            pltpu.SemaphoreType.DMA((2,)),
        ],
        name='layer_front',
    )(idx, x, gain, cosine, sine, w_query, w_key, w_value, kv_heads)


def half_masks(shape, dtype):
    lane = lax.broadcasted_iota(jnp.int32, shape, 1)
    low = jnp.where(lane < 64, 1.0, 0.0)
    return low.astype(dtype), (1.0 - low).astype(dtype)


def block_diag(pair, low, high):
    return jnp.concatenate([pair * low, pair * high], axis=0)


def dot_t(a, b):
    return lax.dot_general(a, b, (((1,), (1,)), ((), ())), preferred_element_type=F32)


def layer_kernel(layer, group, scale, q_ref, k_ref, v_ref, x_ref, gain_ref, kv_hbm, wo_hbm, wg_hbm, wu_hbm, wd_hbm, out_ref,
                 kv, qbuf, obuf, loc, home, score, prob, rowwise, mid, peer_mid, normed, total, peer_total, wo, slab_in, slab_out,
                 kv_sem, q_send, q_recv, o_send, o_recv, wo_sem, sems, peer_send, peer_recv):
    pairs, tokens, lanes = q_ref.shape
    half = pairs // 2
    rows = tokens // CHUNKS
    me = lax.axis_index('pool')
    right, left = lax.rem(me + 1, group), lax.rem(me + group - 1, group)
    toward = (right, left)

    barrier = pltpu.get_barrier_semaphore()
    for neighbour in toward:
        pl.semaphore_signal(barrier, inc=1, device_id={'pool': neighbour}, device_id_type=pl.DeviceIdType.MESH)
    pl.semaphore_wait(barrier, 2)

    def request_at(d, s):
        return lax.rem(me - s + group, group) if d == 0 else lax.rem(me + s, group)

    def kv_copy(d, s):
        return pltpu.make_async_copy(kv_hbm.at[request_at(d, s), :, pl.ds(half * d, half)], kv.at[d, s], kv_sem.at[d, s])

    def q_copy(d, s):
        return pltpu.make_async_remote_copy(
            src_ref=qbuf.at[d, s], dst_ref=qbuf.at[d, s + 1], send_sem=q_send.at[d, s], recv_sem=q_recv.at[d, s + 1],
            device_id={'pool': toward[d]}, device_id_type=pl.DeviceIdType.MESH)

    def q_first(d):
        return pltpu.make_async_remote_copy(
            src_ref=q_ref.at[pl.ds(half * d, half)], dst_ref=qbuf.at[d, 1], send_sem=q_send.at[d, 0], recv_sem=q_recv.at[d, 1],
            device_id={'pool': toward[d]}, device_id_type=pl.DeviceIdType.MESH)

    def o_copy(d, s, c):
        return pltpu.make_async_remote_copy(
            src_ref=obuf.at[d, s - 2, c], dst_ref=obuf.at[d, s - 1, c], send_sem=o_send.at[d, s - 2, c], recv_sem=o_recv.at[d, s - 1, c],
            device_id={'pool': toward[d]}, device_id_type=pl.DeviceIdType.MESH)

    for d in range(2):
        q_first(d).start()

    @pl.loop(0, group)
    def _(s):
        for d in range(2):
            kv_copy(d, s).start()

    depth, tile = slab_out.shape[0], slab_out.shape[1]
    tiles = wg_hbm.shape[2] // tile
    wo_tiles, wo_tile = wo.shape[0], wo.shape[2]

    def read_out(t):
        return pltpu.make_async_copy(wo_hbm.at[layer, :, pl.ds(t * wo_tile, wo_tile)], wo.at[t], wo_sem.at[t])

    core = lax.rem(me, 2)
    peer = me + 1 - 2 * core
    most = (tiles + 1) // 2
    first, count = core * most, most - core * (2 * most - tiles)

    def to_peer(i, src, dst):
        return pltpu.make_async_remote_copy(
            src_ref=src, dst_ref=dst, send_sem=peer_send.at[i], recv_sem=peer_recv.at[i],
            device_id={'pool': peer}, device_id_type=pl.DeviceIdType.MESH)

    def reads(n):
        slot = lax.rem(n, depth)
        t = first + n
        cols = pl.ds(pl.multiple_of(t * tile, tile), tile)
        return (pltpu.make_async_copy(wg_hbm.at[layer, :, cols], slab_in.at[slot, 0], sems.at[slot, 0]),
                pltpu.make_async_copy(wu_hbm.at[layer, :, cols], slab_in.at[slot, 1], sems.at[slot, 1]),
                pltpu.make_async_copy(wd_hbm.at[layer, cols, :], slab_out.at[slot], sems.at[slot, 2]))

    for t in range(wo_tiles):
        read_out(t).start()
    for t in range(depth):
        for copy in reads(t):
            copy.start()

    low_b, high_b = half_masks((tokens, lanes), BF16)

    row_lane = lax.broadcasted_iota(jnp.int32, (rows, lanes), 1)
    row_low = row_lane < 64
    row_at = lax.broadcasted_iota(jnp.int32, (rows, lanes), 0)

    def local_part(d, dest, query_at, key_at, val_at, causal):
        for j in range(half):
            score[d, j] = dot_t(query_at(j), block_diag(key_at(j), low_b, high_b)) * scale
        for c in range(CHUNKS):
            here = slice(c * rows, (c + 1) * rows)
            tops = jnp.zeros((rows, lanes), F32)
            sums = jnp.ones((rows, lanes), F32)
            for j in range(half):
                part = score[d, j, here]
                if causal:
                    part = jnp.where(lax.rem(row_lane, 64) <= row_at + c * rows, part, -1e30)
                top0 = jnp.max(jnp.where(row_low, part, -jnp.inf), axis=1, keepdims=True)
                top1 = jnp.max(jnp.where(row_low, -jnp.inf, part), axis=1, keepdims=True)
                raised = jnp.exp(part - jnp.where(row_low, top0, top1))
                sum0 = jnp.sum(jnp.where(row_low, raised, 0.0), axis=1, keepdims=True)
                sum1 = jnp.sum(jnp.where(row_low, 0.0, raised), axis=1, keepdims=True)
                prob[d, j, here] = (raised * (1.0 / jnp.where(row_low, sum0, sum1))).astype(BF16)
                at0, at1 = row_lane == j, row_lane == 64 + j
                tops = jnp.where(at0, top0, jnp.where(at1, top1, tops))
                sums = jnp.where(at0, sum0, jnp.where(at1, sum1, sums))
            dest[d, c, half] = tops + jnp.log(sums)
        for j in range(half):
            out = jnp.dot(prob[d, j], block_diag(val_at(j), low_b, high_b), preferred_element_type=F32)
            for c in range(CHUNKS):
                dest[d, c, j] = out[c * rows:(c + 1) * rows]

    def weights(far, near):
        gap = far - near
        joint = jnp.maximum(far, near) + jnp.log(1.0 + jnp.exp(-jnp.abs(gap)))
        return 1.0 / (1.0 + jnp.exp(-gap)), joint

    def spread(stat, j):
        return jnp.where(row_low, stat[:, j:j + 1], stat[:, 64 + j:65 + j])

    def merge(d, c, far, near):
        weight, joint = weights(far[half], near[half])
        outs = [near[j] + spread(weight, j) * (far[j] - near[j]) for j in range(half)]
        return outs, joint

    for d in range(2):
        kv_copy(d, 0).wait()
        own = half * d
        local_part(d, home, lambda j: q_ref[own + j], lambda j: kv[d, 0, 0, j], lambda j: kv[d, 0, 1, j], False)
        local_part(d, loc, lambda j: q_ref[own + j], lambda j: k_ref[own + j], lambda j: v_ref[own + j], True)
        for c in range(CHUNKS):
            outs, joint = merge(d, c, home.at[d, c], loc.at[d, c])
            for j in range(half):
                home[d, c, j] = outs[j]
            home[d, c, half] = joint

    def step(s, _):
        for d in range(2):
            q_copy(d, s - 1).wait_recv()

            @pl.when(s < group - 1)
            def _():
                q_copy(d, s).start()

        for d in range(2):
            kv_copy(d, s).wait()
            local_part(d, loc, lambda j: qbuf[d, s, j], lambda j: kv[d, s, 0, j], lambda j: kv[d, s, 1, j], False)

        @pl.when(s == 1)
        def _():
            for d in range(2):
                for c in range(CHUNKS):
                    obuf[d, 0, c] = loc[d, c]

        for c in range(CHUNKS):
            for d in range(2):
                @pl.when(s > 1)
                def _():
                    o_copy(d, s, c).wait_recv()
                    outs, joint = merge(d, c, obuf.at[d, s - 1, c], loc.at[d, c])
                    for j in range(half):
                        obuf[d, s - 1, c, j] = outs[j]
                    obuf[d, s - 1, c, half] = joint

                o_copy(d, s + 1, c).start()
        return 0

    lax.fori_loop(1, group, step, 0)

    for c in range(CHUNKS):
        for d in range(2):
            o_copy(d, group, c).wait_recv()
            outs, _ = merge(d, c, obuf.at[d, group - 1, c], home.at[d, c])
            for j in range(half):
                at = (half * d + j) * lanes
                rowwise[c * rows:(c + 1) * rows, at:at + lanes] = outs[j].astype(BF16)

    for t in range(wo_tiles):
        read_out(t).wait()
        cols = slice(t * wo_tile, (t + 1) * wo_tile)
        proj = jnp.dot(rowwise[...], wo[t], preferred_element_type=F32)
        mid[:, cols] = (x_ref[:, cols].astype(F32) + proj).astype(BF16)
    share = to_peer(0, mid, peer_mid)
    share.start()
    normed[:tokens] = rms_norm(mid[...], gain_ref[...])
    total[...] = jnp.zeros_like(total)
    share.wait_recv()
    normed[tokens:] = rms_norm(peer_mid[...], gain_ref[...])

    def one(n, _):
        slot = lax.rem(n, depth)
        gate_read, up_read, down_read = reads(n)
        gate_read.wait()
        gate = jnp.dot(normed[...], slab_in[slot, 0], preferred_element_type=F32)
        up_read.wait()
        upper = jnp.dot(normed[...], slab_in[slot, 1], preferred_element_type=F32)
        inner = (jax.nn.silu(gate) * upper).astype(BF16)
        down_read.wait()
        total[...] += jnp.dot(inner, slab_out[slot], preferred_element_type=F32)

        @pl.when(n + depth < count)
        def _():
            for copy in reads(n + depth):
                copy.start()

        return 0

    lax.fori_loop(0, count, one, 0)
    back = to_peer(1, total.at[pl.ds(tokens, tokens)], peer_total)
    back.start()
    back.wait_recv()
    out_ref[...] = (mid[...].astype(F32) + (total[:tokens] + peer_total[...])).astype(BF16)
    share.wait_send()
    back.wait_send()

    for d in range(2):
        q_first(d).wait_send()

    @pl.loop(1, group)
    def _(s):
        for d in range(2):
            @pl.when(s < group - 1)
            def _():
                q_copy(d, s).wait_send()

            for c in range(CHUNKS):
                o_copy(d, s + 1, c).wait_send()


def layer_rest(x, query, key, val, packed, gain, w_out, w_gate, w_up, w_down, layer, group, scale, tile=384, depth=4, wo_tile=768):
    pairs, tokens, lanes = query.shape
    width, attn, inner = x.shape[1], w_out.shape[1], w_gate.shape[2]
    half = pairs // 2
    rows = tokens // CHUNKS
    sem = pltpu.SemaphoreType.DMA
    vmem, hbm = pl.BlockSpec(memory_space=pltpu.VMEM), pl.BlockSpec(memory_space=pl.ANY)
    scratch = [
        pltpu.VMEM((2, group, 2, half, tokens, lanes), BF16),
        pltpu.VMEM((2, group, half, tokens, lanes), BF16),
        pltpu.VMEM((2, group, CHUNKS, half + 1, rows, lanes), F32),
        pltpu.VMEM((2, CHUNKS, half + 1, rows, lanes), F32),
        pltpu.VMEM((2, CHUNKS, half + 1, rows, lanes), F32),
        pltpu.VMEM((2, half, tokens, lanes), F32),
        pltpu.VMEM((2, half, tokens, lanes), BF16),
        pltpu.VMEM((tokens, attn), BF16),
        pltpu.VMEM((tokens, width), BF16),
        pltpu.VMEM((tokens, width), BF16),
        pltpu.VMEM((2 * tokens, width), BF16),
        pltpu.VMEM((2 * tokens, width), F32),
        pltpu.VMEM((tokens, width), F32),
        pltpu.VMEM((width // wo_tile, attn, wo_tile), BF16),
        pltpu.VMEM((depth, 2, width, tile), BF16),
        pltpu.VMEM((depth, tile, width), BF16),
        sem((2, group)),
        sem((2, group)),
        sem((2, group)),
        sem((2, group, CHUNKS)),
        sem((2, group, CHUNKS)),
        sem((width // wo_tile,)),
        sem((depth, 3)),
        sem((2,)),
        sem((2,)),
    ]
    return pl.pallas_call(
        functools.partial(layer_kernel, layer, group, scale),
        out_shape=jax.ShapeDtypeStruct(x.shape, BF16),
        in_specs=[vmem] * 5 + [hbm] * 5,
        out_specs=vmem,
        scratch_shapes=scratch,
        compiler_params=pltpu.CompilerParams(collective_id=layer, has_side_effects=True, vmem_limit_bytes=67_000_000),
        name='layer_rest',
    )(query, key, val, x, gain, packed, w_out, w_gate, w_up, w_down)


def solution(mesh):
    group = mesh.shape['pool']

    def local_program(kv_local, idx_local, hid_local, attn_norm, w_query, w_key, w_value, w_out, mlp_norm, w_gate, w_up, w_down):
        layers, _, _, page_len, _, dim = kv_local.shape
        prefix = group * idx_local.shape[2] * page_len
        cosine, sine = rope_tables(prefix, hid_local.shape[1], dim)
        idx = idx_local[:, 0, :]
        kv_heads = jnp.transpose(kv_local, (0, 1, 2, 4, 3, 5))
        x = hid_local[0]
        for layer in range(layers):
            query, key, val, packed = layer_front(
                x, idx, attn_norm[layer:layer + 1], cosine, sine, w_query, w_key, w_value, kv_heads, layer)
            x = layer_rest(x, query, key, val, packed, mlp_norm[layer:layer + 1], w_out, w_gate, w_up, w_down, layer, group, dim ** -0.5)
        return x[None]

    data_specs = (P(None, ('rep', 'pool')), P(None, ('rep', 'pool'), None), P(('rep', 'pool')))
    return jax.shard_map(local_program, mesh=mesh, in_specs=data_specs + (P(),) * 9, out_specs=P(('rep', 'pool')), check_vma=False)
```

```python
import functools
import jax
import jax.numpy as jnp
from jax import lax
from jax.experimental import pallas as pl
from jax.experimental.pallas import tpu as pltpu
from jax.sharding import PartitionSpec as P

NORM_EPS = 1e-6
ROPE_BASE = 10000.0
CHUNKS = 4
F32 = jnp.float32
BF16 = jnp.bfloat16


def rope_tables(offset, tokens, head_dim):
    positions = (offset + jnp.arange(tokens)).astype(F32)
    exponent = jnp.arange(head_dim // 2).astype(F32) * (-2.0 / head_dim)
    inv_freq = jnp.power(ROPE_BASE, exponent)
    angles = positions[:, None] * inv_freq[None, :]
    cosine, sine = jnp.cos(angles), jnp.sin(angles)
    return jnp.concatenate([cosine] * 4, axis=1), jnp.concatenate([-sine, sine] * 2, axis=1)


def rms_norm(vals, gain):
    vals_f = vals.astype(F32)
    inv_rms = lax.rsqrt(jnp.mean(vals_f * vals_f, axis=-1, keepdims=True) + NORM_EPS)
    return (vals_f * inv_rms * gain.astype(F32)).astype(BF16)


def front_kernel(layer, idx_ref, x_ref, gain_ref, cos_ref, sin_ref, wq_hbm, wk_hbm, wv_hbm, kv_hbm,
                 q_ref, k_ref, v_ref, packed_hbm, normed, slab, pages, block, sems, page_sems, out_sems):
    depth, tile = slab.shape[0], slab.shape[3]
    tiles = wq_hbm.shape[2] // tile
    weights = (wq_hbm, wk_hbm, wv_hbm)
    ahead, slots, page_len = pages.shape[0], pages.shape[1], pages.shape[4]
    reqs, pairs = idx_ref.shape[0], block.shape[2]

    def read(t, i):
        slot = lax.rem(t, depth)
        cols = pl.ds(pl.multiple_of(t * tile, tile), tile)
        return pltpu.make_async_copy(weights[i].at[layer, :, cols], slab.at[slot, i], sems.at[slot, i])

    def read_page(r, j):
        slot = lax.rem(r, ahead)
        return pltpu.make_async_copy(kv_hbm.at[layer, idx_ref[r, j]], pages.at[slot, j], page_sems.at[slot, j])

    def write(r):
        slot = lax.rem(r, 2)
        return pltpu.make_async_copy(block.at[slot], packed_hbm.at[r], out_sems.at[slot])

    for t in range(depth):
        for i in range(3):
            read(t, i).start()
    for r in range(ahead):
        for j in range(slots):
            read_page(r, j).start()

    normed[...] = rms_norm(x_ref[...], gain_ref[layer:layer + 1])
    lane = lax.broadcasted_iota(jnp.int32, cos_ref.shape, 1)
    low = (lane % 64) < 32

    def pack(r):
        slot, out_slot = lax.rem(r, ahead), lax.rem(r, 2)

        @pl.when(r >= 2)
        def _():
            write(r - 2).wait()

        for j in range(slots):
            read_page(r, j).wait()
        for j in range(slots):
            rows = pl.ds(j * page_len, page_len)
            for part in range(2):
                for i in range(pairs):
                    both = jnp.concatenate([pages[slot, j, part, 2 * i], pages[slot, j, part, 2 * i + 1]], axis=-1)
                    block[out_slot, part, i, rows, :] = both
        write(r).start()

        @pl.when(r + ahead < reqs)
        def _():
            for j in range(slots):
                read_page(r + ahead, j).start()

    per = -(-reqs // tiles)

    def project(t, _):
        slot = lax.rem(t, depth)
        for i, out_ref in enumerate((q_ref, k_ref, v_ref)):
            read(t, i).wait()
            proj = jnp.dot(normed[...], slab[slot, i], preferred_element_type=F32)
            for p in range(tile // 128):
                part = proj[:, p * 128:(p + 1) * 128]
                if i < 2:
                    swapped = jnp.where(low, pltpu.roll(part, 96, 1), pltpu.roll(part, 32, 1))
                    part = part * cos_ref[...] + swapped * sin_ref[...]
                out_ref[t * (tile // 128) + p] = part.astype(BF16)

            @pl.when(t + depth < tiles)
            def _():
                read(t + depth, i).start()

        for n in range(per):
            r = t * per + n

            @pl.when(r < reqs)
            def _():
                pack(r)

        return 0

    lax.fori_loop(0, tiles, project, 0)
    for r in (reqs - 2, reqs - 1):
        write(r).wait()


def layer_front(x, idx, gain, cosine, sine, w_query, w_key, w_value, kv_heads, layer, tile=256, depth=4, ahead=8):
    tokens, width = x.shape
    cols = w_query.shape[2]
    _, _, _, heads, page_len, dim = kv_heads.shape
    reqs, slots = idx.shape
    block = (2, heads // 2, slots * page_len, 2 * dim)
    vmem, hbm = pl.BlockSpec(memory_space=pltpu.VMEM), pl.BlockSpec(memory_space=pl.ANY)
    out = jax.ShapeDtypeStruct((cols // 128, tokens, 128), BF16)
    return pl.pallas_call(
        functools.partial(front_kernel, layer),
        in_specs=[pl.BlockSpec(memory_space=pltpu.SMEM)] + [vmem] * 4 + [hbm] * 4,
        out_specs=[vmem] * 3 + [hbm],
        out_shape=[out] * 3 + [jax.ShapeDtypeStruct((reqs,) + block, BF16)],
        scratch_shapes=[
            pltpu.VMEM((tokens, width), BF16),
            pltpu.VMEM((depth, 3, width, tile), BF16),
            pltpu.VMEM((ahead, slots, 2, heads, page_len, dim), BF16),
            pltpu.VMEM((2,) + block, BF16),
            pltpu.SemaphoreType.DMA((depth, 3)),
            pltpu.SemaphoreType.DMA((ahead, slots)),
            pltpu.SemaphoreType.DMA((2,)),
        ],
        name='layer_front',
    )(idx, x, gain, cosine, sine, w_query, w_key, w_value, kv_heads)


def half_masks(shape, dtype):
    lane = lax.broadcasted_iota(jnp.int32, shape, 1)
    low = jnp.where(lane < 64, 1.0, 0.0)
    return low.astype(dtype), (1.0 - low).astype(dtype)


def block_diag(pair, low, high):
    return jnp.concatenate([pair * low, pair * high], axis=0)


def dot_t(a, b):
    return lax.dot_general(a, b, (((1,), (1,)), ((), ())), preferred_element_type=F32)


def layer_kernel(layer, group, scale, q_ref, k_ref, v_ref, x_ref, gain_ref, kv_hbm, wo_hbm, wg_hbm, wu_hbm, wd_hbm, out_ref,
                 kv, qbuf, obuf, sbuf, loc, home, stat, share_w, score, prob, rowwise, mid, peer_mid, normed, total, peer_total, wo, slab_in, slab_out,
                 kv_sem, q_send, q_recv, s_send, s_recv, o_send, o_recv, wo_sem, sems, peer_send, peer_recv):
    pairs, tokens, lanes = q_ref.shape
    half = pairs // 2
    rows = tokens // CHUNKS
    me = lax.axis_index('pool')
    right, left = lax.rem(me + 1, group), lax.rem(me + group - 1, group)
    toward = (right, left)

    barrier = pltpu.get_barrier_semaphore()
    for neighbour in toward:
        pl.semaphore_signal(barrier, inc=1, device_id={'pool': neighbour}, device_id_type=pl.DeviceIdType.MESH)
    pl.semaphore_wait(barrier, 2)

    def request_at(d, s):
        return lax.rem(me - s + group, group) if d == 0 else lax.rem(me + s, group)

    def kv_copy(d, s):
        return pltpu.make_async_copy(kv_hbm.at[request_at(d, s), :, pl.ds(half * d, half)], kv.at[d, s], kv_sem.at[d, s])

    def q_copy(d, s):
        return pltpu.make_async_remote_copy(
            src_ref=qbuf.at[d, s], dst_ref=qbuf.at[d, s + 1], send_sem=q_send.at[d, s], recv_sem=q_recv.at[d, s + 1],
            device_id={'pool': toward[d]}, device_id_type=pl.DeviceIdType.MESH)

    def q_first(d):
        return pltpu.make_async_remote_copy(
            src_ref=q_ref.at[pl.ds(half * d, half)], dst_ref=qbuf.at[d, 1], send_sem=q_send.at[d, 0], recv_sem=q_recv.at[d, 1],
            device_id={'pool': toward[d]}, device_id_type=pl.DeviceIdType.MESH)

    def o_copy(d, s, c):
        return pltpu.make_async_remote_copy(
            src_ref=obuf.at[d, s - 2, c], dst_ref=obuf.at[d, s - 1, c], send_sem=o_send.at[d, s - 2, c], recv_sem=o_recv.at[d, s - 1, c],
            device_id={'pool': toward[d]}, device_id_type=pl.DeviceIdType.MESH)

    def s_copy(d, s):
        return pltpu.make_async_remote_copy(
            src_ref=sbuf.at[d, s - 2], dst_ref=sbuf.at[d, s - 1], send_sem=s_send.at[d, s - 2], recv_sem=s_recv.at[d, s - 1],
            device_id={'pool': toward[d]}, device_id_type=pl.DeviceIdType.MESH)

    for d in range(2):
        q_first(d).start()

    @pl.loop(0, group)
    def _(s):
        for d in range(2):
            kv_copy(d, s).start()

    depth, tile = slab_out.shape[0], slab_out.shape[1]
    tiles = wg_hbm.shape[2] // tile
    wo_tiles, wo_tile = wo.shape[0], wo.shape[2]

    def read_out(t):
        return pltpu.make_async_copy(wo_hbm.at[layer, :, pl.ds(t * wo_tile, wo_tile)], wo.at[t], wo_sem.at[t])

    core = lax.rem(me, 2)
    peer = me + 1 - 2 * core
    most = (tiles + 1) // 2
    first, count = core * most, most - core * (2 * most - tiles)

    def to_peer(i, src, dst):
        return pltpu.make_async_remote_copy(
            src_ref=src, dst_ref=dst, send_sem=peer_send.at[i], recv_sem=peer_recv.at[i],
            device_id={'pool': peer}, device_id_type=pl.DeviceIdType.MESH)

    def reads(n):
        slot = lax.rem(n, depth)
        t = first + n
        cols = pl.ds(pl.multiple_of(t * tile, tile), tile)
        return (pltpu.make_async_copy(wg_hbm.at[layer, :, cols], slab_in.at[slot, 0], sems.at[slot, 0]),
                pltpu.make_async_copy(wu_hbm.at[layer, :, cols], slab_in.at[slot, 1], sems.at[slot, 1]),
                pltpu.make_async_copy(wd_hbm.at[layer, cols, :], slab_out.at[slot], sems.at[slot, 2]))

    for t in range(wo_tiles):
        read_out(t).start()
    for t in range(depth):
        for copy in reads(t):
            copy.start()

    low_b, high_b = half_masks((tokens, lanes), BF16)

    row_lane = lax.broadcasted_iota(jnp.int32, (rows, lanes), 1)
    row_low = row_lane < 64
    row_at = lax.broadcasted_iota(jnp.int32, (rows, lanes), 0)

    def local_part(d, dest, which, query_at, key_at, val_at, causal):
        for j in range(half):
            score[d, j] = dot_t(query_at(j), block_diag(key_at(j), low_b, high_b)) * scale
        tops = jnp.zeros((rows, lanes), F32)
        sums = jnp.ones((rows, lanes), F32)
        for c in range(CHUNKS):
            here = slice(c * rows, (c + 1) * rows)
            for j in range(half):
                part = score[d, j, here]
                if causal:
                    part = jnp.where(lax.rem(row_lane, 64) <= row_at + c * rows, part, -1e30)
                top0 = jnp.max(jnp.where(row_low, part, -jnp.inf), axis=1, keepdims=True)
                top1 = jnp.max(jnp.where(row_low, -jnp.inf, part), axis=1, keepdims=True)
                raised = jnp.exp(part - jnp.where(row_low, top0, top1))
                sum0 = jnp.sum(jnp.where(row_low, raised, 0.0), axis=1, keepdims=True)
                sum1 = jnp.sum(jnp.where(row_low, 0.0, raised), axis=1, keepdims=True)
                prob[d, j, here] = (raised * (1.0 / jnp.where(row_low, sum0, sum1))).astype(BF16)
                at0, at1 = row_lane == 16 * c + j, row_lane == 64 + 16 * c + j
                tops = jnp.where(at0, top0, jnp.where(at1, top1, tops))
                sums = jnp.where(at0, sum0, jnp.where(at1, sum1, sums))
        stat[which, d] = tops + jnp.log(sums)
        for j in range(half):
            out = jnp.dot(prob[d, j], block_diag(val_at(j), low_b, high_b), preferred_element_type=F32)
            for c in range(CHUNKS):
                dest[d, c, j] = out[c * rows:(c + 1) * rows]

    def weights(far, near):
        gap = far - near
        joint = jnp.maximum(far, near) + jnp.log(1.0 + jnp.exp(-jnp.abs(gap)))
        return 1.0 / (1.0 + jnp.exp(-gap)), joint

    def merge(d, c, far, near):
        weight = share_w[d]
        at = 16 * c
        outs = []
        for j in range(half):
            spread = jnp.where(row_low, weight[:, at + j:at + j + 1], weight[:, 64 + at + j:65 + at + j])
            outs.append(near[j] + spread * (far[j] - near[j]))
        return outs

    for d in range(2):
        kv_copy(d, 0).wait()
        own = half * d
        local_part(d, home, 0, lambda j: q_ref[own + j], lambda j: kv[d, 0, 0, j], lambda j: kv[d, 0, 1, j], False)
        local_part(d, loc, 1, lambda j: q_ref[own + j], lambda j: k_ref[own + j], lambda j: v_ref[own + j], True)
        share_w[d], stat[0, d] = weights(stat[0, d], stat[1, d])
        for c in range(CHUNKS):
            outs = merge(d, c, home.at[d, c], loc.at[d, c])
            for j in range(half):
                home[d, c, j] = outs[j]

    def step(s, _):
        for d in range(2):
            q_copy(d, s - 1).wait_recv()

            @pl.when(s < group - 1)
            def _():
                q_copy(d, s).start()

        for d in range(2):
            kv_copy(d, s).wait()
            local_part(d, loc, 1, lambda j: qbuf[d, s, j], lambda j: kv[d, s, 0, j], lambda j: kv[d, s, 1, j], False)

        for d in range(2):
            @pl.when(s == 1)
            def _():
                sbuf[d, 0] = stat[1, d]

            @pl.when(s > 1)
            def _():
                s_copy(d, s).wait_recv()
                share_w[d], sbuf[d, s - 1] = weights(sbuf[d, s - 1], stat[1, d])

            s_copy(d, s + 1).start()

        @pl.when(s == 1)
        def _():
            for d in range(2):
                for c in range(CHUNKS):
                    obuf[d, 0, c] = loc[d, c]

        for c in range(CHUNKS):
            for d in range(2):
                @pl.when(s > 1)
                def _():
                    o_copy(d, s, c).wait_recv()
                    outs = merge(d, c, obuf.at[d, s - 1, c], loc.at[d, c])
                    for j in range(half):
                        obuf[d, s - 1, c, j] = outs[j]

                o_copy(d, s + 1, c).start()
        return 0

    lax.fori_loop(1, group, step, 0)

    for d in range(2):
        s_copy(d, group).wait_recv()
        share_w[d], _ = weights(sbuf[d, group - 1], stat[0, d])
    for c in range(CHUNKS):
        for d in range(2):
            o_copy(d, group, c).wait_recv()
            outs = merge(d, c, obuf.at[d, group - 1, c], home.at[d, c])
            for j in range(half):
                at = (half * d + j) * lanes
                rowwise[c * rows:(c + 1) * rows, at:at + lanes] = outs[j].astype(BF16)

    for t in range(wo_tiles):
        read_out(t).wait()
        cols = slice(t * wo_tile, (t + 1) * wo_tile)
        proj = jnp.dot(rowwise[...], wo[t], preferred_element_type=F32)
        mid[:, cols] = (x_ref[:, cols].astype(F32) + proj).astype(BF16)
    share = to_peer(0, mid, peer_mid)
    share.start()
    normed[:tokens] = rms_norm(mid[...], gain_ref[layer:layer + 1])
    total[...] = jnp.zeros_like(total)
    share.wait_recv()
    normed[tokens:] = rms_norm(peer_mid[...], gain_ref[layer:layer + 1])

    def one(n, _):
        slot = lax.rem(n, depth)
        gate_read, up_read, down_read = reads(n)
        gate_read.wait()
        gate = jnp.dot(normed[...], slab_in[slot, 0], preferred_element_type=F32)
        up_read.wait()
        upper = jnp.dot(normed[...], slab_in[slot, 1], preferred_element_type=F32)
        inner = (jax.nn.silu(gate) * upper).astype(BF16)
        down_read.wait()
        total[...] += jnp.dot(inner, slab_out[slot], preferred_element_type=F32)

        @pl.when(n + depth < count)
        def _():
            for copy in reads(n + depth):
                copy.start()

        return 0

    lax.fori_loop(0, count, one, 0)
    back = to_peer(1, total.at[pl.ds(tokens, tokens)], peer_total)
    back.start()
    back.wait_recv()
    out_ref[...] = (mid[...].astype(F32) + (total[:tokens] + peer_total[...])).astype(BF16)
    share.wait_send()
    back.wait_send()

    for d in range(2):
        q_first(d).wait_send()

    @pl.loop(1, group)
    def _(s):
        for d in range(2):
            @pl.when(s < group - 1)
            def _():
                q_copy(d, s).wait_send()

            s_copy(d, s + 1).wait_send()
            for c in range(CHUNKS):
                o_copy(d, s + 1, c).wait_send()


def layer_rest(x, query, key, val, packed, gain, w_out, w_gate, w_up, w_down, layer, group, scale, tile=384, depth=4, wo_tile=768):
    pairs, tokens, lanes = query.shape
    width, attn, inner = x.shape[1], w_out.shape[1], w_gate.shape[2]
    half = pairs // 2
    rows = tokens // CHUNKS
    sem = pltpu.SemaphoreType.DMA
    vmem, hbm = pl.BlockSpec(memory_space=pltpu.VMEM), pl.BlockSpec(memory_space=pl.ANY)
    scratch = [
        pltpu.VMEM((2, group, 2, half, tokens, lanes), BF16),
        pltpu.VMEM((2, group, half, tokens, lanes), BF16),
        pltpu.VMEM((2, group, CHUNKS, half, rows, lanes), F32),
        pltpu.VMEM((2, group, rows, lanes), F32),
        pltpu.VMEM((2, CHUNKS, half, rows, lanes), F32),
        pltpu.VMEM((2, CHUNKS, half, rows, lanes), F32),
        pltpu.VMEM((2, 2, rows, lanes), F32),
        pltpu.VMEM((2, rows, lanes), F32),
        pltpu.VMEM((2, half, tokens, lanes), F32),
        pltpu.VMEM((2, half, tokens, lanes), BF16),
        pltpu.VMEM((tokens, attn), BF16),
        pltpu.VMEM((tokens, width), BF16),
        pltpu.VMEM((tokens, width), BF16),
        pltpu.VMEM((2 * tokens, width), BF16),
        pltpu.VMEM((2 * tokens, width), F32),
        pltpu.VMEM((tokens, width), F32),
        pltpu.VMEM((width // wo_tile, attn, wo_tile), BF16),
        pltpu.VMEM((depth, 2, width, tile), BF16),
        pltpu.VMEM((depth, tile, width), BF16),
        sem((2, group)),
        sem((2, group)),
        sem((2, group)),
        sem((2, group)),
        sem((2, group)),
        sem((2, group, CHUNKS)),
        sem((2, group, CHUNKS)),
        sem((width // wo_tile,)),
        sem((depth, 3)),
        sem((2,)),
        sem((2,)),
    ]
    return pl.pallas_call(
        functools.partial(layer_kernel, layer, group, scale),
        out_shape=jax.ShapeDtypeStruct(x.shape, BF16),
        in_specs=[vmem] * 5 + [hbm] * 5,
        out_specs=vmem,
        scratch_shapes=scratch,
        compiler_params=pltpu.CompilerParams(collective_id=layer, has_side_effects=True, vmem_limit_bytes=67_000_000),
        name='layer_rest',
    )(query, key, val, x, gain, packed, w_out, w_gate, w_up, w_down)


def solution(mesh):
    group = mesh.shape['pool']

    def local_program(kv_local, idx_local, hid_local, attn_norm, w_query, w_key, w_value, w_out, mlp_norm, w_gate, w_up, w_down):
        layers, _, _, page_len, _, dim = kv_local.shape
        prefix = group * idx_local.shape[2] * page_len
        cosine, sine = rope_tables(prefix, hid_local.shape[1], dim)
        idx = idx_local[:, 0, :]
        kv_heads = jnp.transpose(kv_local, (0, 1, 2, 4, 3, 5))
        x = hid_local[0]
        for layer in range(layers):
            query, key, val, packed = layer_front(
                x, idx, attn_norm, cosine, sine, w_query, w_key, w_value, kv_heads, layer)
            x = layer_rest(x, query, key, val, packed, mlp_norm, w_out, w_gate, w_up, w_down, layer, group, dim ** -0.5)
        return x[None]

    data_specs = (P(None, ('rep', 'pool')), P(None, ('rep', 'pool'), None), P(('rep', 'pool')))
    return jax.shard_map(local_program, mesh=mesh, in_specs=data_specs + (P(),) * 9, out_specs=P(('rep', 'pool')), check_vma=False)
```

```python
import functools
import jax
import jax.numpy as jnp
from jax import lax
from jax.experimental import pallas as pl
from jax.experimental.pallas import tpu as pltpu
from jax.sharding import PartitionSpec as P

NORM_EPS = 1e-6
ROPE_BASE = 10000.0
CHUNKS = 4
F32 = jnp.float32
BF16 = jnp.bfloat16


def rope_tables(offset, tokens, head_dim):
    positions = (offset + jnp.arange(tokens)).astype(F32)
    exponent = jnp.arange(head_dim // 2).astype(F32) * (-2.0 / head_dim)
    inv_freq = jnp.power(ROPE_BASE, exponent)
    angles = positions[:, None] * inv_freq[None, :]
    cosine, sine = jnp.cos(angles), jnp.sin(angles)
    return jnp.concatenate([cosine] * 4, axis=1), jnp.concatenate([-sine, sine] * 2, axis=1)


def rms_norm(vals, gain):
    vals_f = vals.astype(F32)
    inv_rms = lax.rsqrt(jnp.mean(vals_f * vals_f, axis=-1, keepdims=True) + NORM_EPS)
    return (vals_f * inv_rms * gain.astype(F32)).astype(BF16)


def front_kernel(layer, idx_ref, x_ref, gain_ref, cos_ref, sin_ref, wq_hbm, wk_hbm, wv_hbm, kv_hbm,
                 q_ref, k_ref, v_ref, packed_hbm, normed, slab, pages, block, sems, page_sems, out_sems):
    depth, tile = slab.shape[0], slab.shape[3]
    tiles = wq_hbm.shape[2] // tile
    weights = (wq_hbm, wk_hbm, wv_hbm)
    ahead, slots, page_len = pages.shape[0], pages.shape[1], pages.shape[4]
    reqs, pairs = idx_ref.shape[0], block.shape[2]

    def read(t, i):
        slot = lax.rem(t, depth)
        cols = pl.ds(pl.multiple_of(t * tile, tile), tile)
        return pltpu.make_async_copy(weights[i].at[layer, :, cols], slab.at[slot, i], sems.at[slot, i])

    def read_page(r, j):
        slot = lax.rem(r, ahead)
        return pltpu.make_async_copy(kv_hbm.at[layer, idx_ref[r, j]], pages.at[slot, j], page_sems.at[slot, j])

    def write(r):
        slot = lax.rem(r, 2)
        return pltpu.make_async_copy(block.at[slot], packed_hbm.at[r], out_sems.at[slot])

    for t in range(depth):
        for i in range(3):
            read(t, i).start()
    for r in range(ahead):
        for j in range(slots):
            read_page(r, j).start()

    normed[...] = rms_norm(x_ref[...], gain_ref[layer:layer + 1])
    lane = lax.broadcasted_iota(jnp.int32, cos_ref.shape, 1)
    low = (lane % 64) < 32

    def pack(r):
        slot, out_slot = lax.rem(r, ahead), lax.rem(r, 2)

        @pl.when(r >= 2)
        def _():
            write(r - 2).wait()

        for j in range(slots):
            read_page(r, j).wait()
        for j in range(slots):
            rows = pl.ds(j * page_len, page_len)
            for part in range(2):
                for i in range(pairs):
                    both = jnp.concatenate([pages[slot, j, part, 2 * i], pages[slot, j, part, 2 * i + 1]], axis=-1)
                    block[out_slot, part, i, rows, :] = both
        write(r).start()

        @pl.when(r + ahead < reqs)
        def _():
            for j in range(slots):
                read_page(r + ahead, j).start()

    per = -(-reqs // tiles)

    def project(t, _):
        slot = lax.rem(t, depth)
        for i, out_ref in enumerate((q_ref, k_ref, v_ref)):
            read(t, i).wait()
            proj = jnp.dot(normed[...], slab[slot, i], preferred_element_type=F32)
            for p in range(tile // 128):
                part = proj[:, p * 128:(p + 1) * 128]
                if i < 2:
                    swapped = jnp.where(low, pltpu.roll(part, 96, 1), pltpu.roll(part, 32, 1))
                    part = part * cos_ref[...] + swapped * sin_ref[...]
                out_ref[t * (tile // 128) + p] = part.astype(BF16)

            @pl.when(t + depth < tiles)
            def _():
                read(t + depth, i).start()

        for n in range(per):
            r = t * per + n

            @pl.when(r < reqs)
            def _():
                pack(r)

        return 0

    lax.fori_loop(0, tiles, project, 0)
    for r in (reqs - 2, reqs - 1):
        write(r).wait()


def layer_front(x, idx, gain, cosine, sine, w_query, w_key, w_value, kv_heads, layer, tile=256, depth=4, ahead=8):
    tokens, width = x.shape
    cols = w_query.shape[2]
    _, _, _, heads, page_len, dim = kv_heads.shape
    reqs, slots = idx.shape
    block = (2, heads // 2, slots * page_len, 2 * dim)
    vmem, hbm = pl.BlockSpec(memory_space=pltpu.VMEM), pl.BlockSpec(memory_space=pl.ANY)
    out = jax.ShapeDtypeStruct((cols // 128, tokens, 128), BF16)
    return pl.pallas_call(
        functools.partial(front_kernel, layer),
        in_specs=[pl.BlockSpec(memory_space=pltpu.SMEM)] + [vmem] * 4 + [hbm] * 4,
        out_specs=[vmem] * 3 + [hbm],
        out_shape=[out] * 3 + [jax.ShapeDtypeStruct((reqs,) + block, BF16)],
        scratch_shapes=[
            pltpu.VMEM((tokens, width), BF16),
            pltpu.VMEM((depth, 3, width, tile), BF16),
            pltpu.VMEM((ahead, slots, 2, heads, page_len, dim), BF16),
            pltpu.VMEM((2,) + block, BF16),
            pltpu.SemaphoreType.DMA((depth, 3)),
            pltpu.SemaphoreType.DMA((ahead, slots)),
            pltpu.SemaphoreType.DMA((2,)),
        ],
        name='layer_front',
    )(idx, x, gain, cosine, sine, w_query, w_key, w_value, kv_heads)


def half_masks(shape, dtype):
    lane = lax.broadcasted_iota(jnp.int32, shape, 1)
    low = jnp.where(lane < 64, 1.0, 0.0)
    return low.astype(dtype), (1.0 - low).astype(dtype)


def block_diag(pair, low, high):
    return jnp.concatenate([pair * low, pair * high], axis=0)


def dot_t(a, b):
    return lax.dot_general(a, b, (((1,), (1,)), ((), ())), preferred_element_type=F32)


def layer_kernel(layer, group, scale, q_ref, k_ref, v_ref, x_ref, gain_ref, kv_hbm, wo_hbm, wg_hbm, wu_hbm, wd_hbm, out_ref,
                 kv, qbuf, obuf, sbuf, loc, home, stat, share_w, score, prob, rowwise, mid, peer_mid, normed, total, peer_total, wo, slab_in, slab_out,
                 kv_sem, q_send, q_recv, s_send, s_recv, o_send, o_recv, wo_sem, sems, peer_send, peer_recv):
    pairs, tokens, lanes = q_ref.shape
    half = pairs // 2
    rows = tokens // CHUNKS
    me = lax.axis_index('pool')
    right, left = lax.rem(me + 1, group), lax.rem(me + group - 1, group)
    toward = (right, left)

    barrier = pltpu.get_barrier_semaphore()
    for neighbour in toward:
        pl.semaphore_signal(barrier, inc=1, device_id={'pool': neighbour}, device_id_type=pl.DeviceIdType.MESH)
    pl.semaphore_wait(barrier, 2)

    def request_at(d, s):
        return lax.rem(me - s + group, group) if d == 0 else lax.rem(me + s, group)

    def kv_copy(d, s):
        return pltpu.make_async_copy(kv_hbm.at[request_at(d, s), :, pl.ds(half * d, half)], kv.at[d, s], kv_sem.at[d, s])

    def q_copy(d, s):
        return pltpu.make_async_remote_copy(
            src_ref=qbuf.at[d, s], dst_ref=qbuf.at[d, s + 1], send_sem=q_send.at[d, s], recv_sem=q_recv.at[d, s + 1],
            device_id={'pool': toward[d]}, device_id_type=pl.DeviceIdType.MESH)

    def q_first(d):
        return pltpu.make_async_remote_copy(
            src_ref=q_ref.at[pl.ds(half * d, half)], dst_ref=qbuf.at[d, 1], send_sem=q_send.at[d, 0], recv_sem=q_recv.at[d, 1],
            device_id={'pool': toward[d]}, device_id_type=pl.DeviceIdType.MESH)

    def o_copy(d, s, c):
        return pltpu.make_async_remote_copy(
            src_ref=obuf.at[d, s - 2, c], dst_ref=obuf.at[d, s - 1, c], send_sem=o_send.at[d, s - 2, c], recv_sem=o_recv.at[d, s - 1, c],
            device_id={'pool': toward[d]}, device_id_type=pl.DeviceIdType.MESH)

    def s_copy(d, s):
        return pltpu.make_async_remote_copy(
            src_ref=sbuf.at[d, s - 2], dst_ref=sbuf.at[d, s - 1], send_sem=s_send.at[d, s - 2], recv_sem=s_recv.at[d, s - 1],
            device_id={'pool': toward[d]}, device_id_type=pl.DeviceIdType.MESH)

    for d in range(2):
        q_first(d).start()

    @pl.loop(0, group)
    def _(s):
        for d in range(2):
            kv_copy(d, s).start()

    depth, tile = slab_out.shape[0], slab_out.shape[1]
    tiles = wg_hbm.shape[2] // tile
    wo_tiles, wo_tile = wo.shape[0], wo.shape[2]

    def read_out(t):
        return pltpu.make_async_copy(wo_hbm.at[layer, :, pl.ds(t * wo_tile, wo_tile)], wo.at[t], wo_sem.at[t])

    core = lax.rem(me, 2)
    peer = me + 1 - 2 * core
    most = (tiles + 1) // 2
    first, count = core * most, most - core * (2 * most - tiles)

    def to_peer(i, src, dst):
        return pltpu.make_async_remote_copy(
            src_ref=src, dst_ref=dst, send_sem=peer_send.at[i], recv_sem=peer_recv.at[i],
            device_id={'pool': peer}, device_id_type=pl.DeviceIdType.MESH)

    def reads(n):
        slot = lax.rem(n, depth)
        t = first + n
        cols = pl.ds(pl.multiple_of(t * tile, tile), tile)
        return (pltpu.make_async_copy(wg_hbm.at[layer, :, cols], slab_in.at[slot, 0], sems.at[slot, 0]),
                pltpu.make_async_copy(wu_hbm.at[layer, :, cols], slab_in.at[slot, 1], sems.at[slot, 1]),
                pltpu.make_async_copy(wd_hbm.at[layer, cols, :], slab_out.at[slot], sems.at[slot, 2]))

    for t in range(wo_tiles):
        read_out(t).start()
    for t in range(depth):
        for copy in reads(t):
            copy.start()

    low_b, high_b = half_masks((tokens, lanes), BF16)

    row_lane = lax.broadcasted_iota(jnp.int32, (rows, lanes), 1)
    row_low = row_lane < 64
    row_at = lax.broadcasted_iota(jnp.int32, (rows, lanes), 0)

    def local_part(d, dest, which, query_at, key_at, val_at, causal):
        for j in range(half):
            score[d, j] = dot_t(query_at(j), block_diag(key_at(j), low_b, high_b)) * scale
        tops = jnp.zeros((rows, lanes), F32)
        sums = jnp.ones((rows, lanes), F32)
        for c in range(CHUNKS):
            here = slice(c * rows, (c + 1) * rows)
            for j in range(half):
                part = score[d, j, here]
                if causal:
                    part = jnp.where(lax.rem(row_lane, 64) <= row_at + c * rows, part, -1e30)
                top0 = jnp.max(jnp.where(row_low, part, -jnp.inf), axis=1, keepdims=True)
                top1 = jnp.max(jnp.where(row_low, -jnp.inf, part), axis=1, keepdims=True)
                raised = jnp.exp(part - jnp.where(row_low, top0, top1))
                sum0 = jnp.sum(jnp.where(row_low, raised, 0.0), axis=1, keepdims=True)
                sum1 = jnp.sum(jnp.where(row_low, 0.0, raised), axis=1, keepdims=True)
                prob[d, j, here] = (raised * (1.0 / jnp.where(row_low, sum0, sum1))).astype(BF16)
                at0, at1 = row_lane == 16 * c + j, row_lane == 64 + 16 * c + j
                tops = jnp.where(at0, top0, jnp.where(at1, top1, tops))
                sums = jnp.where(at0, sum0, jnp.where(at1, sum1, sums))
        stat[which, d] = tops + jnp.log(sums)
        for j in range(half):
            out = jnp.dot(prob[d, j], block_diag(val_at(j), low_b, high_b), preferred_element_type=F32)
            for c in range(CHUNKS):
                dest[d, c, j] = out[c * rows:(c + 1) * rows]

    def weights(far, near):
        gap = far - near
        joint = jnp.maximum(far, near) + jnp.log(1.0 + jnp.exp(-jnp.abs(gap)))
        return 1.0 / (1.0 + jnp.exp(-gap)), joint

    def merge(d, c, far, near):
        weight = share_w[d]
        at = 16 * c
        outs = []
        for j in range(half):
            spread = jnp.where(row_low, weight[:, at + j:at + j + 1], weight[:, 64 + at + j:65 + at + j])
            outs.append(near[j] + spread * (far[j] - near[j]))
        return outs

    def home_part(d):
        kv_copy(d, 0).wait()
        own = half * d
        local_part(d, home, 0, lambda j: q_ref[own + j], lambda j: kv[d, 0, 0, j], lambda j: kv[d, 0, 1, j], False)
        local_part(d, loc, 1, lambda j: q_ref[own + j], lambda j: k_ref[own + j], lambda j: v_ref[own + j], True)
        share_w[d], stat[0, d] = weights(stat[0, d], stat[1, d])
        for c in range(CHUNKS):
            outs = merge(d, c, home.at[d, c], loc.at[d, c])
            for j in range(half):
                home[d, c, j] = outs[j]

    def step(s, _):
        for d in range(2):
            q_copy(d, s - 1).wait_recv()

            @pl.when(s < group - 1)
            def _():
                q_copy(d, s).start()

        for d in range(2):
            kv_copy(d, s).wait()
            local_part(d, loc, 1, lambda j: qbuf[d, s, j], lambda j: kv[d, s, 0, j], lambda j: kv[d, s, 1, j], False)

        for d in range(2):
            @pl.when(s == 1)
            def _():
                sbuf[d, 0] = stat[1, d]

            @pl.when(s > 1)
            def _():
                s_copy(d, s).wait_recv()
                share_w[d], sbuf[d, s - 1] = weights(sbuf[d, s - 1], stat[1, d])

            s_copy(d, s + 1).start()

        @pl.when(s == 1)
        def _():
            for d in range(2):
                for c in range(CHUNKS):
                    obuf[d, 0, c] = loc[d, c]

        for c in range(CHUNKS):
            for d in range(2):
                @pl.when(s > 1)
                def _():
                    o_copy(d, s, c).wait_recv()
                    outs = merge(d, c, obuf.at[d, s - 1, c], loc.at[d, c])
                    for j in range(half):
                        obuf[d, s - 1, c, j] = outs[j]

                o_copy(d, s + 1, c).start()

        for d in range(2):
            @pl.when(s == 4 + 3 * d)
            def _():
                home_part(d)

        return 0

    lax.fori_loop(1, group, step, 0)

    for d in range(2):
        s_copy(d, group).wait_recv()
        share_w[d], _ = weights(sbuf[d, group - 1], stat[0, d])
    for c in range(CHUNKS):
        for d in range(2):
            o_copy(d, group, c).wait_recv()
            outs = merge(d, c, obuf.at[d, group - 1, c], home.at[d, c])
            for j in range(half):
                at = (half * d + j) * lanes
                rowwise[c * rows:(c + 1) * rows, at:at + lanes] = outs[j].astype(BF16)

    for t in range(wo_tiles):
        read_out(t).wait()
        cols = slice(t * wo_tile, (t + 1) * wo_tile)
        proj = jnp.dot(rowwise[...], wo[t], preferred_element_type=F32)
        mid[:, cols] = (x_ref[:, cols].astype(F32) + proj).astype(BF16)
    share = to_peer(0, mid, peer_mid)
    share.start()
    normed[:tokens] = rms_norm(mid[...], gain_ref[layer:layer + 1])
    total[...] = jnp.zeros_like(total)
    share.wait_recv()
    normed[tokens:] = rms_norm(peer_mid[...], gain_ref[layer:layer + 1])

    def one(n, _):
        slot = lax.rem(n, depth)
        gate_read, up_read, down_read = reads(n)
        gate_read.wait()
        gate = jnp.dot(normed[...], slab_in[slot, 0], preferred_element_type=F32)
        up_read.wait()
        upper = jnp.dot(normed[...], slab_in[slot, 1], preferred_element_type=F32)
        inner = (jax.nn.silu(gate) * upper).astype(BF16)
        down_read.wait()
        total[...] += jnp.dot(inner, slab_out[slot], preferred_element_type=F32)

        @pl.when(n + depth < count)
        def _():
            for copy in reads(n + depth):
                copy.start()

        return 0

    lax.fori_loop(0, count, one, 0)
    back = to_peer(1, total.at[pl.ds(tokens, tokens)], peer_total)
    back.start()
    back.wait_recv()
    out_ref[...] = (mid[...].astype(F32) + (total[:tokens] + peer_total[...])).astype(BF16)
    share.wait_send()
    back.wait_send()

    for d in range(2):
        q_first(d).wait_send()

    @pl.loop(1, group)
    def _(s):
        for d in range(2):
            @pl.when(s < group - 1)
            def _():
                q_copy(d, s).wait_send()

            s_copy(d, s + 1).wait_send()
            for c in range(CHUNKS):
                o_copy(d, s + 1, c).wait_send()


def layer_rest(x, query, key, val, packed, gain, w_out, w_gate, w_up, w_down, layer, group, scale, tile=384, depth=4, wo_tile=768):
    pairs, tokens, lanes = query.shape
    width, attn, inner = x.shape[1], w_out.shape[1], w_gate.shape[2]
    half = pairs // 2
    rows = tokens // CHUNKS
    sem = pltpu.SemaphoreType.DMA
    vmem, hbm = pl.BlockSpec(memory_space=pltpu.VMEM), pl.BlockSpec(memory_space=pl.ANY)
    scratch = [
        pltpu.VMEM((2, group, 2, half, tokens, lanes), BF16),
        pltpu.VMEM((2, group, half, tokens, lanes), BF16),
        pltpu.VMEM((2, group, CHUNKS, half, rows, lanes), F32),
        pltpu.VMEM((2, group, rows, lanes), F32),
        pltpu.VMEM((2, CHUNKS, half, rows, lanes), F32),
        pltpu.VMEM((2, CHUNKS, half, rows, lanes), F32),
        pltpu.VMEM((2, 2, rows, lanes), F32),
        pltpu.VMEM((2, rows, lanes), F32),
        pltpu.VMEM((2, half, tokens, lanes), F32),
        pltpu.VMEM((2, half, tokens, lanes), BF16),
        pltpu.VMEM((tokens, attn), BF16),
        pltpu.VMEM((tokens, width), BF16),
        pltpu.VMEM((tokens, width), BF16),
        pltpu.VMEM((2 * tokens, width), BF16),
        pltpu.VMEM((2 * tokens, width), F32),
        pltpu.VMEM((tokens, width), F32),
        pltpu.VMEM((width // wo_tile, attn, wo_tile), BF16),
        pltpu.VMEM((depth, 2, width, tile), BF16),
        pltpu.VMEM((depth, tile, width), BF16),
        sem((2, group)),
        sem((2, group)),
        sem((2, group)),
        sem((2, group)),
        sem((2, group)),
        sem((2, group, CHUNKS)),
        sem((2, group, CHUNKS)),
        sem((width // wo_tile,)),
        sem((depth, 3)),
        sem((2,)),
        sem((2,)),
    ]
    return pl.pallas_call(
        functools.partial(layer_kernel, layer, group, scale),
        out_shape=jax.ShapeDtypeStruct(x.shape, BF16),
        in_specs=[vmem] * 5 + [hbm] * 5,
        out_specs=vmem,
        scratch_shapes=scratch,
        compiler_params=pltpu.CompilerParams(collective_id=layer, has_side_effects=True, vmem_limit_bytes=67_000_000),
        name='layer_rest',
    )(query, key, val, x, gain, packed, w_out, w_gate, w_up, w_down)


def solution(mesh):
    group = mesh.shape['pool']

    def local_program(kv_local, idx_local, hid_local, attn_norm, w_query, w_key, w_value, w_out, mlp_norm, w_gate, w_up, w_down):
        layers, _, _, page_len, _, dim = kv_local.shape
        prefix = group * idx_local.shape[2] * page_len
        cosine, sine = rope_tables(prefix, hid_local.shape[1], dim)
        idx = idx_local[:, 0, :]
        kv_heads = jnp.transpose(kv_local, (0, 1, 2, 4, 3, 5))
        x = hid_local[0]
        for layer in range(layers):
            query, key, val, packed = layer_front(
                x, idx, attn_norm, cosine, sine, w_query, w_key, w_value, kv_heads, layer)
            x = layer_rest(x, query, key, val, packed, mlp_norm, w_out, w_gate, w_up, w_down, layer, group, dim ** -0.5)
        return x[None]

    data_specs = (P(None, ('rep', 'pool')), P(None, ('rep', 'pool'), None), P(('rep', 'pool')))
    return jax.shard_map(local_program, mesh=mesh, in_specs=data_specs + (P(),) * 9, out_specs=P(('rep', 'pool')), check_vma=False)
```
